128 devices in a mesh: dp: 1, tp: 2 (over core), sp: 64 (over z, y, x).
Axes of the slice: x: 4, y: 4, z: 4, core: 2. Of those that a mesh axis runs over, the one named last changes fastest.
Arguments:
- hidden: bfloat16 [32, 5120], P('dp')
- lat_cache: bfloat16 [32, 16384, 512], P('dp', 'sp')
- rope_cache: bfloat16 [32, 16384, 64], P('dp', 'sp')
- positions: int32 [32], P('dp')
- w_dq: bfloat16 [5120, 1536], replicated
- gain_q: bfloat16 [1536], replicated
- w_dkv: bfloat16 [5120, 576], replicated
- gain_kv: bfloat16 [512], replicated
- w_uq: bfloat16 [1536, 128, 192], P(None, 'tp')
- w_uk: bfloat16 [512, 128, 128], P(None, 'tp')
- w_uv: bfloat16 [512, 128, 128], P(None, 'tp')
- w_out: bfloat16 [16384, 5120], P('tp')
Outputs:
- output 1: bfloat16 [32, 5120], P('dp')
- output 2: bfloat16 [32, 16384, 512], P('dp', 'sp')
- output 3: bfloat16 [32, 16384, 64], P('dp', 'sp')
All inputs are finite; a program needn't handle non-finite values.
Results may differ from the reference program's by a relative error of at most 0.00918123.
Values sent between devices are 32-bit elements.
A program may use at most 1 GiB of HBM per device.

```python
import math
import jax
import jax.numpy as jnp
from jax import lax

BATCH = 32
SEQ = 16384
DMODEL = 5120
HEADS = 128
QRANK = 1536
KVRANK = 512
NOPE = 128
ROPE = 64
VHEAD = 128

EPSILON = 1e-6
ROPE_BASE = 50000.0
SCORE_SCALE = (1.0 + 0.1 * math.log(32.0)) ** 2 / math.sqrt(NOPE + ROPE)
LAT_SPREAD = 1.2
ROPE_SPREAD = 1.7


def setup_inputs(seed: int = 0, part: int = 0) -> dict:
    base_key = jax.random.key(seed)
    shared_keys = jax.random.split(base_key, 8)
    part_keys = jax.random.split(jax.random.fold_in(base_key, part), 5)
    hidden = jax.random.normal(part_keys[0], (BATCH, DMODEL), jnp.float32)
    lat_cache = LAT_SPREAD * jax.random.normal(part_keys[1], (BATCH, SEQ, KVRANK), jnp.float32)
    rope_cache = ROPE_SPREAD * jax.random.normal(part_keys[2], (BATCH, SEQ, ROPE), jnp.float32)
    long_pos = jax.random.randint(part_keys[3], (BATCH,), 0, SEQ, jnp.int32)
    short_pos = jax.random.randint(part_keys[4], (BATCH,), 0, 4, jnp.int32)
    positions = jnp.where(jnp.arange(BATCH) % 4 == 1, short_pos, long_pos)
    positions = positions.at[0].set(SEQ - 1).at[1].set(0)
    w_dq = jax.random.normal(shared_keys[0], (DMODEL, QRANK), jnp.float32) * DMODEL ** -0.5
    gain_q = 1.0 + 0.5 * jax.random.normal(shared_keys[1], (QRANK,), jnp.float32)
    w_dkv = jax.random.normal(shared_keys[2], (DMODEL, KVRANK + ROPE), jnp.float32) * DMODEL ** -0.5
    gain_kv = 1.0 + 0.5 * jax.random.normal(shared_keys[3], (KVRANK,), jnp.float32)
    w_uq = jax.random.normal(shared_keys[4], (QRANK, HEADS, NOPE + ROPE), jnp.float32) * QRANK ** -0.5
    w_uk = jax.random.normal(shared_keys[5], (KVRANK, HEADS, NOPE), jnp.float32) * KVRANK ** -0.5
    w_uv = jax.random.normal(shared_keys[6], (KVRANK, HEADS, VHEAD), jnp.float32) * KVRANK ** -0.5
    w_out = jax.random.normal(shared_keys[7], (HEADS * VHEAD, DMODEL), jnp.float32) * (HEADS * VHEAD) ** -0.5
    return {
        'hidden': hidden.astype(jnp.bfloat16),
        'lat_cache': lat_cache.astype(jnp.bfloat16),
        'rope_cache': rope_cache.astype(jnp.bfloat16),
        'positions': positions,
        'w_dq': w_dq.astype(jnp.bfloat16),
        'gain_q': gain_q.astype(jnp.bfloat16),
        'w_dkv': w_dkv.astype(jnp.bfloat16),
        'gain_kv': gain_kv.astype(jnp.bfloat16),
        'w_uq': w_uq.astype(jnp.bfloat16),
        'w_uk': w_uk.astype(jnp.bfloat16),
        'w_uv': w_uv.astype(jnp.bfloat16),
        'w_out': w_out.astype(jnp.bfloat16),
    }


def rms_norm(values, gain):
    vals32 = values.astype(jnp.float32)
    inv_rms = lax.rsqrt(jnp.mean(vals32 * vals32, axis=-1, keepdims=True) + EPSILON)
    return vals32 * inv_rms * gain.astype(jnp.float32)


def rope_angles(positions):
    half_dim = ROPE // 2
    inv_freq = ROPE_BASE ** (-jnp.arange(half_dim).astype(jnp.float32) / half_dim)
    return positions.astype(jnp.float32)[:, None] * inv_freq[None, :]


def rotate_pairs(values, cos_t, sin_t):
    half_dim = values.shape[-1] // 2
    first_half = values[..., :half_dim]
    second_half = values[..., half_dim:]
    return jnp.concatenate([first_half * cos_t - second_half * sin_t, second_half * cos_t + first_half * sin_t], axis=-1)


def attend_one(operands):
    q_abs, q_rope, lat_all, rope_all, position = operands
    lat32 = lat_all.astype(jnp.float32)
    scores = (jnp.einsum('hk,sk->hs', q_abs.astype(jnp.float32), lat32) + jnp.einsum('hr,sr->hs', q_rope.astype(jnp.float32), rope_all.astype(jnp.float32))) * SCORE_SCALE
    key_valid = jnp.arange(SEQ)[None, :] <= position
    scores = jnp.where(key_valid, scores, -jnp.inf)
    probs = jax.nn.softmax(scores, axis=-1)
    return jnp.einsum('hs,sk->hk', probs, lat32).astype(jnp.bfloat16)


def reference(hidden, lat_cache, rope_cache, positions, w_dq, gain_q, w_dkv, gain_kv, w_uq, w_uk, w_uv, w_out):
    angles = rope_angles(positions)
    cos_t = jnp.cos(angles)
    sin_t = jnp.sin(angles)
    h_q = jnp.dot(hidden, w_dq, preferred_element_type=jnp.float32).astype(jnp.bfloat16)
    c_q = rms_norm(h_q, gain_q).astype(jnp.bfloat16)
    q_full = jnp.einsum('br,rhd->bhd', c_q.astype(jnp.float32), w_uq.astype(jnp.float32)).astype(jnp.bfloat16)
    q_nope = q_full[:, :, :NOPE]
    q_rope = rotate_pairs(q_full[:, :, NOPE:].astype(jnp.float32), cos_t[:, None, :], sin_t[:, None, :]).astype(jnp.bfloat16)
    kv_down = jnp.dot(hidden, w_dkv, preferred_element_type=jnp.float32).astype(jnp.bfloat16)
    lat_new = rms_norm(kv_down[:, :KVRANK], gain_kv).astype(jnp.bfloat16)
    rope_new = rotate_pairs(kv_down[:, KVRANK:].astype(jnp.float32), cos_t, sin_t).astype(jnp.bfloat16)
    slot_hit = (jnp.arange(SEQ)[None, :] == positions[:, None])[:, :, None]
    lat_all = jnp.where(slot_hit, lat_new[:, None, :], lat_cache)
    rope_all = jnp.where(slot_hit, rope_new[:, None, :], rope_cache)
    q_abs = jnp.einsum('bhn,khn->bhk', q_nope.astype(jnp.float32), w_uk.astype(jnp.float32)).astype(jnp.bfloat16)
    o_lat = lax.map(attend_one, (q_abs, q_rope, lat_all, rope_all, positions))
    o_heads = jnp.einsum('bhk,khv->bhv', o_lat.astype(jnp.float32), w_uv.astype(jnp.float32)).astype(jnp.bfloat16)
    attn_out = jnp.dot(o_heads.reshape(BATCH, HEADS * VHEAD), w_out, preferred_element_type=jnp.float32)
    return (hidden.astype(jnp.float32) + attn_out).astype(jnp.bfloat16), lat_all, rope_all
```

```python
import math
import jax
import jax.numpy as jnp
from jax import lax
from jax.experimental import pallas as pl
from jax.experimental.pallas import tpu as pltpu
from jax.sharding import PartitionSpec as P

EPSILON = 1e-6
ROPE_BASE = 50000.0
YARN_MSCALE = 1.0 + 0.1 * math.log(32.0)
MASK_VALUE = -1e30
MESH = pl.DeviceIdType.MESH

HEAD_STRIDE = (16, 4, 1)
SP_STRIDE = (1, 4, 16)
ORDERS = ((0, 1, 2), (1, 2, 0), (2, 0, 1))
UNIT_LO = (0, 5, 10)
UNIT_HI = (5, 10, 16)
OUT_LO = (0, 256)
OUT_HI = (256, 640)


def rms_norm(values, gain):
    vals32 = values.astype(jnp.float32)
    inv_rms = lax.rsqrt(jnp.mean(vals32 * vals32, axis=-1, keepdims=True) + EPSILON)
    return vals32 * inv_rms * gain.astype(jnp.float32)


def rope_tables(positions, rope_dim):
    half_dim = rope_dim // 2
    inv_freq = ROPE_BASE ** (-jnp.arange(half_dim).astype(jnp.float32) / half_dim)
    angles = positions.astype(jnp.float32)[:, None] * inv_freq[None, :]
    return jnp.cos(angles), jnp.sin(angles)


def rotate_pairs(values, cos_t, sin_t):
    half_dim = values.shape[-1] // 2
    first_half = values[..., :half_dim]
    second_half = values[..., half_dim:]
    return jnp.concatenate([first_half * cos_t - second_half * sin_t, second_half * cos_t + first_half * sin_t], axis=-1)


def project_inputs(hidden, positions, w_dq, gain_q, w_dkv, gain_kv, w_uq, w_uk):
    kv_rank = w_uk.shape[0]
    nope_dim = w_uk.shape[2]
    cos_t, sin_t = rope_tables(positions, w_uq.shape[2] - nope_dim)
    h_q = jnp.dot(hidden, w_dq, preferred_element_type=jnp.float32).astype(jnp.bfloat16)
    c_q = rms_norm(h_q, gain_q).astype(jnp.bfloat16)
    q_full = jnp.einsum('br,rhd->bhd', c_q, w_uq, preferred_element_type=jnp.float32).astype(jnp.bfloat16)
    q_rope = rotate_pairs(q_full[:, :, nope_dim:].astype(jnp.float32), cos_t[:, None, :], sin_t[:, None, :]).astype(jnp.bfloat16)
    q_abs = jnp.einsum('bhn,khn->bhk', q_full[:, :, :nope_dim], w_uk, preferred_element_type=jnp.float32).astype(jnp.bfloat16)
    kv_down = jnp.dot(hidden, w_dkv, preferred_element_type=jnp.float32).astype(jnp.bfloat16)
    lat_new = rms_norm(kv_down[:, :kv_rank], gain_kv).astype(jnp.bfloat16)
    rope_new = rotate_pairs(kv_down[:, kv_rank:].astype(jnp.float32), cos_t, sin_t).astype(jnp.bfloat16)
    return q_abs, q_rope, lat_new, rope_new


def tail_kernel(u_ref, st_ref, hid_ref, wuv_ref, wout_ref, out_ref,
                r1, v1, r2, v2, r3, s1, s2, q1, q2, q3,
                wuv_v, wuv_h, wout_v, y_buf, y_in, t1, t2, p1, p2, zbuf, g_buf,
                send_sem, recv_sem, load_sem):
    sp = lax.axis_index('sp')
    tp = lax.axis_index('tp')
    coord = (lax.rem(sp, 4), lax.rem(sp // 4, 4), sp // 16)
    head = coord[0] * 16 + coord[1] * 4 + coord[2]
    group = pl.multiple_of((head // 8) * 8, 8)

    load_uv = pltpu.make_async_copy(wuv_ref.at[:, pl.ds(group, 8), :], wuv_v, load_sem.at[0])
    load_uv.start()
    load_out = pltpu.make_async_copy(wout_ref.at[pl.ds(pl.multiple_of(head * 128, 128), 128), :], wout_v, load_sem.at[1])
    load_out.start()

    def peer_coord(axis, step):
        return lax.rem(coord[axis] + step, 4)

    def peer_id(axis, step):
        return {'sp': sp + (peer_coord(axis, step) - coord[axis]) * SP_STRIDE[axis]}

    barrier = pltpu.get_barrier_semaphore()
    for axis in range(3):
        for step in range(1, 4):
            pl.semaphore_signal(barrier, inc=1, device_id=peer_id(axis, step), device_id_type=MESH)
    pl.semaphore_signal(barrier, inc=1, device_id={'tp': 1 - tp}, device_id_type=MESH)
    pl.semaphore_wait(barrier, 10)

    started = []

    def send(src, dst, device):
        index = len(started)
        copy = pltpu.make_async_remote_copy(
            src_ref=src, dst_ref=dst, send_sem=send_sem.at[index], recv_sem=recv_sem.at[index],
            device_id=device, device_id_type=MESH)
        copy.start()
        started.append(copy)
        return copy

    lane = lax.broadcasted_iota(jnp.int32, (2, 8, 128), 2)

    def merge_stats(stats, offset):
        top = jnp.maximum(jnp.maximum(stats[0], stats[1]), jnp.maximum(stats[2], stats[3]))
        shift = lax.rem(128 - offset, 128)
        factors = [jnp.exp(s - top) for s in stats]
        den = sum(f * pltpu.roll(s, 64, 2) for f, s in zip(factors, stats))
        merged = jnp.where(lane < 64, top, pltpu.roll(den, 64, 2))
        return pltpu.roll(merged, shift, 2), [pltpu.roll(f, shift, 2) for f in factors]

    def spread(factor, lane_index):
        return jnp.broadcast_to(factor[:, lane_index:lane_index + 1], (8, 128))

    pending = {}
    for colour in range(3):
        axis = ORDERS[colour][0]
        lo, hi = UNIT_LO[colour], UNIT_HI[colour]
        for step in (2, 1, 3):
            pc = peer_coord(axis, step)
            sel = [slice(None)] * 3
            sel[axis] = pc
            src = u_ref.at[(pl.ds(lo, hi - lo),) + tuple(sel)]
            a = send(src, r1.at[step - 1, pl.ds(lo, hi - lo)], peer_id(axis, step))
            b = send(st_ref.at[pl.ds(colour, 2)], q1.at[colour, step - 1], peer_id(axis, step))
            pending[colour, step] = (a, b)

    load_uv.wait()
    pick = lax.broadcasted_iota(jnp.int32, (64, 8, 128), 1) == lax.rem(head, 8)

    def pick_rows(i, carry):
        rows = pl.ds(pl.multiple_of(i * 64, 64), 64)
        block = wuv_v[rows].astype(jnp.float32)
        wuv_h[rows, :] = jnp.sum(jnp.where(pick, block, 0.0), axis=1).astype(jnp.bfloat16)
        return carry

    lax.fori_loop(0, 8, pick_rows, 0)

    for colour in range(3):
        order = ORDERS[colour]
        axis = order[0]
        lo, hi = UNIT_LO[colour], UNIT_HI[colour]
        for step in (1, 3, 2):
            for copy in pending[colour, step]:
                copy.wait_recv()
        stats = [st_ref[pl.ds(colour, 2)]] + [q1[colour, i] for i in range(3)]
        merged, factors = merge_stats(stats, coord[axis] * HEAD_STRIDE[axis])
        s1[colour] = merged
        first, second = [a for a in range(3) if a != axis]
        own = [slice(None)] * 3
        own[axis] = coord[axis]
        for i in range(4):
            for j in range(4):
                where = HEAD_STRIDE[first] * i + HEAD_STRIDE[second] * j
                at = [None] * 3
                at[axis], at[first], at[second] = coord[axis], i, j
                for bt in range(lo // 4, (hi - 1) // 4 + 1):
                    fb = [spread(f[bt - colour], where) for f in factors]
                    for unit in range(max(lo, bt * 4), min(hi, bt * 4 + 4)):
                        total = fb[0] * u_ref[unit, at[0], at[1], at[2]]
                        for k in range(3):
                            total = total + fb[k + 1] * r1[k, unit, i, j]
                        v1[unit, i, j] = total
        axis2 = order[1]
        for step in (2, 1, 3):
            pc = peer_coord(axis2, step)
            sel = (pc, slice(None)) if axis2 == first else (slice(None), pc)
            a = send(v1.at[(pl.ds(lo, hi - lo),) + sel], r2.at[step - 1, pl.ds(lo, hi - lo)], peer_id(axis2, step))
            b = send(s1.at[colour], q2.at[colour, step - 1], peer_id(axis2, step))
            pending[colour, step] = (a, b)

    for colour in range(3):
        order = ORDERS[colour]
        axis, axis2, axis3 = order
        lo, hi = UNIT_LO[colour], UNIT_HI[colour]
        first, second = [a for a in range(3) if a != axis]
        for step in (1, 3, 2):
            for copy in pending[colour, step]:
                copy.wait_recv()
        stats = [s1[colour]] + [q2[colour, i] for i in range(3)]
        merged, factors = merge_stats(stats, coord[axis2] * HEAD_STRIDE[axis2])
        s2[colour] = merged
        for i in range(4):
            at = (coord[axis2], i) if axis2 == first else (i, coord[axis2])
            for bt in range(lo // 4, (hi - 1) // 4 + 1):
                fb = [spread(f[bt - colour], HEAD_STRIDE[axis3] * i) for f in factors]
                for unit in range(max(lo, bt * 4), min(hi, bt * 4 + 4)):
                    total = fb[0] * v1[unit, at[0], at[1]]
                    for k in range(3):
                        total = total + fb[k + 1] * r2[k, unit, i]
                    v2[unit, i] = total
        for step in (2, 1, 3):
            a = send(v2.at[pl.ds(lo, hi - lo), peer_coord(axis3, step)], r3.at[step - 1, pl.ds(lo, hi - lo)], peer_id(axis3, step))
            b = send(s2.at[colour], q3.at[colour, step - 1], peer_id(axis3, step))
            pending[colour, step] = (a, b)

    units = [None] * 16
    den = [None] * 16
    for colour in range(3):
        axis3 = ORDERS[colour][2]
        lo, hi = UNIT_LO[colour], UNIT_HI[colour]
        for step in (1, 3, 2):
            for copy in pending[colour, step]:
                copy.wait_recv()
        stats = [s2[colour]] + [q3[colour, i] for i in range(3)]
        merged, factors = merge_stats(stats, coord[axis3] * HEAD_STRIDE[axis3])
        for bt in range(lo // 4, (hi - 1) // 4 + 1):
            fb = [spread(f[bt - colour], 0) for f in factors]
            dn = spread(merged[bt - colour], 64)
            for unit in range(max(lo, bt * 4), min(hi, bt * 4 + 4)):
                total = fb[0] * v2[unit, coord[axis3]]
                for k in range(3):
                    total = total + fb[k + 1] * r3[k, unit]
                units[unit] = total / dn
    o_lat = jnp.concatenate(
        [jnp.concatenate([units[bt * 4 + kt] for kt in range(4)], axis=1) for bt in range(4)], axis=0).astype(jnp.bfloat16)
    o_head = jnp.dot(o_lat, wuv_h[...], preferred_element_type=jnp.float32).astype(jnp.bfloat16)
    load_out.wait()
    for half in range(2):
        for cg in range(4):
            base = half * 2560 + cg * 640
            part = jnp.dot(o_head, wout_v[:, base:base + 640], preferred_element_type=jnp.float32)
            for bt in range(4):
                y_buf[half, bt, cg] = part[bt * 8:bt * 8 + 8, :]

    pair = send(y_buf.at[1 - tp], y_in, {'tp': 1 - tp})
    pair.wait_recv()
    for bt in range(4):
        for cg in range(4):
            y_in[bt, cg] = y_in[bt, cg] + y_buf[tp, bt, cg]

    for colour in range(2):
        cols = pl.ds(OUT_LO[colour], OUT_HI[colour] - OUT_LO[colour])
        axis = colour
        for step in (2, 1, 3):
            pc = peer_coord(axis, step)
            src = y_in.at[pc, :, :, cols] if axis == 0 else y_in.at[:, pc, :, cols]
            pending[colour, step] = send(src, t1.at[step - 1, :, :, cols], peer_id(axis, step))
    for colour in range(2):
        cols = pl.ds(OUT_LO[colour], OUT_HI[colour] - OUT_LO[colour])
        axis, axis2 = colour, 1 - colour
        for step in (1, 3, 2):
            pending[colour, step].wait_recv()
        for i in range(4):
            own = y_in[coord[0], i, :, cols] if axis == 0 else y_in[i, coord[1], :, cols]
            p1[i, :, cols] = own + t1[0, i, :, cols] + t1[1, i, :, cols] + t1[2, i, :, cols]
        for step in (2, 1, 3):
            pending[colour, step] = send(
                p1.at[peer_coord(axis2, step), :, cols], t2.at[step - 1, :, cols], peer_id(axis2, step))
    for colour in range(2):
        cols = pl.ds(OUT_LO[colour], OUT_HI[colour] - OUT_LO[colour])
        axis2 = 1 - colour
        for step in (1, 3, 2):
            pending[colour, step].wait_recv()
        p2[:, cols] = p1[coord[axis2], :, cols] + t2[0, :, cols] + t2[1, :, cols] + t2[2, :, cols]

    for step in (2, 1, 3):
        pending[0, step] = send(p2, zbuf.at[coord[2]], peer_id(2, step))
    zbuf[coord[2]] = p2[...]
    for step in (1, 3, 2):
        pending[0, step].wait_recv()
    g_buf[tp, coord[0], coord[1]] = (zbuf[0] + zbuf[1]) + (zbuf[2] + zbuf[3])

    for colour in range(2):
        cols = pl.ds(OUT_LO[colour], OUT_HI[colour] - OUT_LO[colour])
        axis2 = 1 - colour
        mine = g_buf.at[tp, coord[0], coord[1], :, cols]
        for step in (2, 1, 3):
            pending[colour, step] = send(mine, mine, peer_id(axis2, step))
    for colour in range(2):
        cols = pl.ds(OUT_LO[colour], OUT_HI[colour] - OUT_LO[colour])
        axis = colour
        for step in (1, 3, 2):
            pending[colour, step].wait_recv()
        mine = g_buf.at[tp, coord[0], :, :, cols] if axis == 0 else g_buf.at[tp, :, coord[1], :, cols]
        for step in (2, 1, 3):
            pending[colour, step] = send(mine, mine, peer_id(axis, step))
    for colour in range(2):
        for step in (1, 3, 2):
            pending[colour, step].wait_recv()
    pair = send(g_buf.at[tp], g_buf.at[tp], {'tp': 1 - tp})
    pair.wait_recv()
    for half in range(2):
        for cg in range(4):
            base = half * 2560 + cg * 640
            full = jnp.concatenate([g_buf[half, bt, cg] for bt in range(4)], axis=0)
            out_ref[:, base:base + 640] = (hid_ref[:, base:base + 640].astype(jnp.float32) + full).astype(jnp.bfloat16)
    for copy in started:
        copy.wait_send()


N_SENDS = 54 + 1 + 12 + 3 + 12 + 1


def tail(u_parts, stats, hidden, w_uv, w_out):
    f32, bf16 = jnp.float32, jnp.bfloat16
    vmem = pl.BlockSpec(memory_space=pltpu.VMEM)
    hbm = pl.BlockSpec(memory_space=pl.ANY)
    return pl.pallas_call(
        tail_kernel,
        out_shape=jax.ShapeDtypeStruct((32, 5120), bf16),
        in_specs=[vmem, vmem, vmem, hbm, hbm],
        out_specs=vmem,
        scratch_shapes=[
            pltpu.VMEM((3, 16, 4, 4, 8, 128), f32),
            pltpu.VMEM((16, 4, 4, 8, 128), f32),
            pltpu.VMEM((3, 16, 4, 8, 128), f32),
            pltpu.VMEM((16, 4, 8, 128), f32),
            pltpu.VMEM((3, 16, 8, 128), f32),
            pltpu.VMEM((3, 2, 8, 128), f32),
            pltpu.VMEM((3, 2, 8, 128), f32),
            pltpu.VMEM((3, 3, 2, 8, 128), f32),
            pltpu.VMEM((3, 3, 2, 8, 128), f32),
            pltpu.VMEM((3, 3, 2, 8, 128), f32),
            pltpu.VMEM((512, 8, 128), bf16),
            pltpu.VMEM((512, 128), bf16),
            pltpu.VMEM((128, 5120), bf16),
            pltpu.VMEM((2, 4, 4, 8, 640), f32),
            pltpu.VMEM((4, 4, 8, 640), f32),
            pltpu.VMEM((3, 4, 8, 640), f32),
            pltpu.VMEM((3, 8, 640), f32),
            pltpu.VMEM((4, 8, 640), f32),
            pltpu.VMEM((8, 640), f32),
            pltpu.VMEM((4, 8, 640), f32),
            pltpu.VMEM((2, 4, 4, 8, 640), f32),
            pltpu.SemaphoreType.DMA((N_SENDS,)),
            pltpu.SemaphoreType.DMA((N_SENDS,)),
            pltpu.SemaphoreType.DMA((2,)),
        ],
        compiler_params=pltpu.CompilerParams(collective_id=0, has_side_effects=True),
        name='tail',
    )(u_parts, stats, hidden, w_uv, w_out)


def solution(mesh):
    row_spec = P('dp', None)
    cache_spec = P('dp', 'sp', None)
    head_spec = P(None, 'tp', None)
    in_specs = (row_spec, cache_spec, cache_spec, P('dp'), P(), P(), P(), P(), head_spec, head_spec, head_spec, P('tp', None))
    out_specs = (row_spec, cache_spec, cache_spec)

    def local_step(hidden, lat_cache, rope_cache, positions, w_dq, gain_q, w_dkv, gain_kv, w_uq, w_uk, w_uv, w_out):
        seq_local = lat_cache.shape[1]
        score_scale = YARN_MSCALE ** 2 / math.sqrt(w_uq.shape[2])
        q_abs, q_rope, lat_new, rope_new = project_inputs(hidden, positions, w_dq, gain_q, w_dkv, gain_kv, w_uq, w_uk)
        slot_ids = lax.axis_index('sp') * seq_local + jnp.arange(seq_local)
        slot_hit = (slot_ids[None, :] == positions[:, None])[:, :, None]
        lat_all = jnp.where(slot_hit, lat_new[:, None, :], lat_cache)
        rope_all = jnp.where(slot_hit, rope_new[:, None, :], rope_cache)
        scores = (jnp.einsum('bhk,bsk->bhs', q_abs, lat_all, preferred_element_type=jnp.float32) + jnp.einsum('bhr,bsr->bhs', q_rope, rope_all, preferred_element_type=jnp.float32)) * score_scale
        key_valid = slot_ids[None, None, :] <= positions[:, None, None]
        scores = jnp.where(key_valid, scores, MASK_VALUE)
        max_local = jnp.max(scores, axis=-1)
        weights = jnp.exp(scores - max_local[:, :, None])
        lat_part = jnp.einsum('bhs,bsk->bhk', weights.astype(jnp.bfloat16), lat_all, preferred_element_type=jnp.float32)
        den_local = jnp.sum(weights, axis=-1)
        stats = jnp.concatenate([max_local, den_local], axis=1).reshape(4, 8, 128)
        u_parts = lat_part.reshape(4, 8, 64, 4, 128).transpose(0, 3, 2, 1, 4).reshape(16, 4, 4, 4, 8, 128)
        out = tail(u_parts, stats, hidden, w_uv, w_out)
        return out, lat_all, rope_all

    return jax.shard_map(local_step, mesh=mesh, in_specs=in_specs, out_specs=out_specs, check_vma=False)
```

```python
import functools
import math
import jax
import jax.numpy as jnp
from jax import lax
from jax.experimental import pallas as pl
from jax.experimental.pallas import tpu as pltpu
from jax.sharding import PartitionSpec as P

EPSILON = 1e-6
ROPE_BASE = 50000.0
YARN_MSCALE = 1.0 + 0.1 * math.log(32.0)
MASK_VALUE = -1e30
TILE = (8, 128)
HEAD_GROUP = 16
UQ_RING = 4
MIB = 2 ** 20
FRONT_VMEM = 48 * MIB
ATTEND_VMEM = 46 * MIB
TAIL_VMEM = 50 * MIB
SEND_ORDER = (2, 1, 3)
WAIT_ORDER = (1, 3, 2)
MESH = pl.DeviceIdType.MESH
NT = (((1,), (1,)), ((), ()))
f32, bf16 = jnp.float32, jnp.bfloat16

HEAD_STRIDE = (16, 4, 1)
SP_STRIDE = (1, 4, 16)
ORDERS = ((0, 1, 2), (1, 2, 0), (2, 0, 1))
UNIT_LO = (0, 5, 10)
UNIT_MID = (2, 8, 13)
UNIT_HI = (5, 10, 16)
RING = (1, 3)
RING_STEPS = (1, 2, 3)
OUT_LO = (0, 256)
OUT_HI = (256, 640)


def rope_tables(positions, rope_dim):
    half_dim = rope_dim // 2
    inv_freq = ROPE_BASE ** (-jnp.arange(half_dim).astype(jnp.float32) / half_dim)
    angles = positions.astype(jnp.float32)[:, None] * inv_freq[None, :]
    return jnp.cos(angles), jnp.sin(angles)


def front_kernel(hid_ref, gq_ref, gkv_ref, cos_ref, sin_ref, wdkv_hbm, wdq_hbm, wuk_hbm, wuq_hbm,
                 qabs_ref, qrope_ref, lnew_ref, rnew_ref, wdkv_v, wdq_v, wuk_v, wuq_v, sem_kv, sem_q, sem_k, sem_u):
    n_kv, n_q, ring = wdkv_v.shape[0], wdq_v.shape[0], wuq_v.shape[0]
    kv_cols, q_rows, part = wdkv_v.shape[2], wdq_v.shape[1], wuq_v.shape[1]
    n_parts = wuq_hbm.shape[0] // part

    def load_uq(i):
        return pltpu.make_async_copy(wuq_hbm.at[pl.ds(i * part, part)], wuq_v.at[i % ring], sem_u.at[i % ring])

    kv_loads = [pltpu.make_async_copy(wdkv_hbm.at[:, pl.ds(i * kv_cols, kv_cols)], wdkv_v.at[i], sem_kv.at[i]) for i in range(n_kv)]
    q_loads = [pltpu.make_async_copy(wdq_hbm.at[pl.ds(i * q_rows, q_rows), :], wdq_v.at[i], sem_q.at[i]) for i in range(n_q)]
    k_rows = wuk_v.shape[0] // 4
    k_loads = [pltpu.make_async_copy(wuk_hbm.at[pl.ds(i * k_rows, k_rows)], wuk_v.at[pl.ds(i * k_rows, k_rows)], sem_k.at[i]) for i in range(4)]
    uq_loads = [load_uq(i) for i in range(n_parts)]
    queue = kv_loads + q_loads + uq_loads[:2] + k_loads + uq_loads[2:]
    state = [0]

    def issue(count):
        for copy in queue[state[0]:state[0] + count]:
            copy.start()
        state[0] += count

    issue(UQ_RING)
    cos_t, sin_t = cos_ref[...], sin_ref[...]
    half = cos_t.shape[1]

    def rotate(v):
        v1, v2 = v[:, :half], v[:, half:]
        return jnp.concatenate([v1 * cos_t - v2 * sin_t, v2 * cos_t + v1 * sin_t], axis=1)

    def norm(values, gain_ref):
        v = values.astype(bf16).astype(f32)
        inv = lax.rsqrt(jnp.mean(v * v, axis=1, keepdims=True) + EPSILON)
        return (v * inv * gain_ref[...].astype(f32)).astype(bf16)

    kv = jnp.zeros((32, wdkv_v.shape[1]), f32)
    for i in range(n_kv):
        kv_loads[i].wait()
        issue(1)
        kv = kv + lax.dot_general(hid_ref[:, i * kv_cols:(i + 1) * kv_cols], wdkv_v[i], NT, preferred_element_type=f32)
    lnew_ref[...] = norm(kv[:, :512], gkv_ref)
    turned = rotate(kv[:, 512:].astype(bf16).astype(f32)).T.astype(bf16)
    for t in range(4):
        rnew_ref[t] = turned[:, t * 8:t * 8 + 8]
    h_q = jnp.zeros((32, 1536), f32)
    for i in range(n_q):
        q_loads[i].wait()
        issue(1)
        h_q = h_q + jnp.dot(hid_ref[:, i * q_rows:(i + 1) * q_rows], wdq_v[i], preferred_element_type=f32)
    cq = norm(h_q, gq_ref)

    nope, rotated = [], []
    zero = jnp.zeros((32, 128), bf16)

    def absorb(group):
        wuk = jnp.swapaxes(wuk_v[:, group * HEAD_GROUP:(group + 1) * HEAD_GROUP, :], 0, 1)
        absorbed = []
        for i in range(0, HEAD_GROUP, 2):
            a, b = nope[group * HEAD_GROUP + i], nope[group * HEAD_GROUP + i + 1]
            pair = jnp.concatenate([jnp.concatenate([a, zero], axis=1), jnp.concatenate([zero, b], axis=1)], axis=0)
            both = lax.dot_general(pair, jnp.concatenate([wuk[i], wuk[i + 1]], axis=1), NT, preferred_element_type=f32)
            absorbed += [both[:32], both[32:]]
        where = slice(group * HEAD_GROUP, (group + 1) * HEAD_GROUP)
        qabs_ref[:, where, :] = jnp.swapaxes(jnp.stack(absorbed), 0, 1).astype(bf16)
        qrope_ref[:, where, :] = jnp.swapaxes(jnp.stack(rotated[where]), 0, 1).astype(bf16)

    per_group = HEAD_GROUP // part
    for i in range(n_parts):
        uq_loads[i].wait()
        w = wuq_v[i % ring].reshape(part * 192, 1536)
        q4 = lax.dot_general(cq, w, NT, preferred_element_type=f32).astype(bf16)
        for j in range(part):
            q = q4[:, j * 192:j * 192 + 192]
            nope.append(q[:, :128])
            rotated.append(rotate(q[:, 128:].astype(f32)))
        issue(1)
        if i == 1:
            for copy in k_loads:
                copy.wait()
                issue(1)
        if i % per_group == per_group - 1:
            absorb(i // per_group)


def front(hidden, gain_q, gain_kv, cos_t, sin_t, w_dkv, w_dq, w_uk, w_uq):
    heads = w_uq.shape[1]
    vmem = pl.BlockSpec(memory_space=pltpu.VMEM)
    hbm = pl.BlockSpec(memory_space=pltpu.HBM)
    dma = pltpu.SemaphoreType.DMA
    shape = jax.ShapeDtypeStruct
    return pl.pallas_call(
        front_kernel,
        out_shape=(shape((32, heads, 512), bf16), shape((32, heads, 64), bf16), shape((32, 512), bf16), shape((4, 64, 8), bf16)),
        in_specs=[vmem] * 5 + [hbm] * 4,
        out_specs=[vmem] * 4,
        scratch_shapes=[
            pltpu.VMEM((4, 576, 1280), bf16),
            pltpu.VMEM((5, 1024, 1536), bf16),
            pltpu.VMEM((512, heads, 128), bf16),
            pltpu.VMEM((UQ_RING, 4, 192, 1536), bf16),
            dma((4,)), dma((5,)), dma((4,)), dma((UQ_RING,)),
        ],
        compiler_params=pltpu.CompilerParams(vmem_limit_bytes=FRONT_VMEM),
        name='front',
    )(hidden, gain_q.reshape(1, -1), gain_kv.reshape(1, -1), cos_t, sin_t, w_dkv.T, w_dq, w_uk, w_uq.transpose(1, 2, 0))


def attend_kernel(base_ref, pos_ref, qabs_ref, qrope_ref, lat_ref, rope_ref, lnew_ref, rnew_ref,
                  lat_out, rope_out, u_ref, st_ref, s_buf, w_buf, *, scale):
    tile = pl.program_id(0)
    base = base_ref[0]
    lane256 = lax.broadcasted_iota(jnp.int32, (64, 256), 1)
    lane128 = lax.broadcasted_iota(jnp.int32, (64, 128), 1)
    row16 = lax.broadcasted_iota(jnp.int32, (16, 512), 0)
    lat_out[...] = lat_ref[...]
    slots = [pos_ref[tile * 8 + b] - base for b in range(8)]
    for b in range(8):
        slot = slots[b]
        group = jnp.clip(slot // 16, 0, 15) * 16
        rows = pl.ds(pl.multiple_of(group, 16), 16)
        new = jnp.broadcast_to(lnew_ref[b:b + 1, :].astype(f32), (16, 512))
        lat_out[b, rows, :] = jnp.where(row16 == slot - group, new, lat_ref[b, rows, :].astype(f32)).astype(bf16)
        rope_out[b] = jnp.where(lane256 == slot, rnew_ref[0, :, b:b + 1].astype(f32), rope_ref[b].astype(f32)).astype(bf16)
    for b in range(8):
        s = lax.dot_general(qabs_ref[tile * 8 + b], lat_out[b], NT, preferred_element_type=f32)
        s_buf[b] = s + jnp.dot(qrope_ref[tile * 8 + b], rope_out[b], preferred_element_type=f32)
    tops = jnp.zeros((64, 128), f32)
    dens = jnp.zeros((64, 128), f32)
    for b in range(8):
        s = jnp.where(lane256 <= slots[b], s_buf[b] * scale, MASK_VALUE)
        top = jnp.max(s, axis=1, keepdims=True)
        w = jnp.exp(s - top)
        den = jnp.sum(w, axis=1, keepdims=True)
        w_buf[b] = w.astype(bf16)
        tops = jnp.where(lane128 == b, top, tops)
        dens = jnp.where(lane128 == b, den, dens)
    st_ref[0] = jnp.concatenate([tops, dens], axis=0).T[:8, :]
    for b in range(8):
        u = jnp.dot(w_buf[b], lat_out[b], preferred_element_type=f32)
        for kt in range(4):
            u_ref[tile * 4 + kt, pl.ds(b, 64, stride=8), :] = u[:, kt * 128:kt * 128 + 128]


def attend(base, positions, q_abs, q_rope, lat_cache, rope_t, lat_new, rope_new, scale):
    vmem = pl.BlockSpec(memory_space=pltpu.VMEM)
    smem = pl.BlockSpec(memory_space=pltpu.SMEM)
    first = lambda t: (t, 0, 0)
    return pl.pallas_call(
        functools.partial(attend_kernel, scale=scale),
        grid=(4,),
        out_shape=(jax.ShapeDtypeStruct((32, 256, 512), bf16), jax.ShapeDtypeStruct((32, 64, 256), bf16),
                   jax.ShapeDtypeStruct((16, 512, 128), f32), jax.ShapeDtypeStruct((4, 8, 128), f32)),
        in_specs=[smem, smem,
                  vmem, vmem,
                  pl.BlockSpec((8, 256, 512), first), pl.BlockSpec((8, 64, 256), first),
                  pl.BlockSpec((8, 512), lambda t: (t, 0)), pl.BlockSpec((1, 64, 8), first)],
        out_specs=[pl.BlockSpec((8, 256, 512), first), pl.BlockSpec((8, 64, 256), first),
                   vmem, pl.BlockSpec((1, 8, 128), first)],
        scratch_shapes=[pltpu.VMEM((8, 64, 256), f32), pltpu.VMEM((8, 64, 256), bf16)],
        compiler_params=pltpu.CompilerParams(vmem_limit_bytes=ATTEND_VMEM),
        name='attend',
    )(base, positions, q_abs, q_rope, lat_cache, rope_t, lat_new, rope_new)


def tail_kernel(u_ref, st_ref, wuv_ref, wout_ref, out_ref,
                relay, passed, r1, v1, r2, v2, r3, s1, s2, q0, q1, q2, q3,
                wuv_v, wuv_h, wout_v, y_buf, y_in, t1, t2, p1, p2, zbuf, g_buf,
                send_sem, recv_sem, load_sem):
    sp = lax.axis_index('sp')
    tp = lax.axis_index('tp')
    coord = (lax.rem(sp, 4), lax.rem(sp // 4, 4), sp // 16)
    x, y, z = coord
    head = x * 16 + y * 4 + z
    group = pl.multiple_of((head // 8) * 8, 8)

    load_uv = pltpu.make_async_copy(wuv_ref.at[:, pl.ds(group, 8), :], wuv_v, load_sem.at[0])
    load_uv.start()
    load_out = pltpu.make_async_copy(wout_ref.at[pl.ds(pl.multiple_of(head * 128, 128), 128), :], wout_v, load_sem.at[1])
    load_out.start()

    def peer_coord(axis, step):
        return lax.rem(coord[axis] + step, 4)

    def peer_id(axis, step):
        return {'sp': sp + (peer_coord(axis, step) - coord[axis]) * SP_STRIDE[axis]}

    barrier = pltpu.get_barrier_semaphore()
    for axis in range(3):
        for step in RING_STEPS:
            pl.semaphore_signal(barrier, inc=1, device_id=peer_id(axis, step), device_id_type=MESH)
    pl.semaphore_signal(barrier, inc=1, device_id={'tp': 1 - tp}, device_id_type=MESH)
    pl.semaphore_wait(barrier, 10)

    started = []

    def send(src, dst, device):
        index = len(started)
        copy = pltpu.make_async_remote_copy(
            src_ref=src, dst_ref=dst, send_sem=send_sem.at[index], recv_sem=recv_sem.at[index],
            device_id=device, device_id_type=MESH)
        copy.start()
        started.append(copy)
        return copy

    lane = lax.broadcasted_iota(jnp.int32, (2, 8, 128), 2)

    def merge_stats(stats, offset, turn_result=True):
        top = functools.reduce(jnp.maximum, stats)
        shift = lax.rem(128 - offset, 128)
        factors = [jnp.exp(s - top) for s in stats]
        den = sum(f * pltpu.roll(s, 64, 2) for f, s in zip(factors, stats))
        merged = jnp.where(lane < 64, top, pltpu.roll(den, 64, 2))
        if turn_result:
            merged = pltpu.roll(merged, shift, 2)
        return merged, [pltpu.roll(f, shift, 2) for f in factors]

    def spread(factor, lane_index):
        return jnp.broadcast_to(factor[:, lane_index:lane_index + 1], (8, 128))

    pending = {}

    def block(axis, position, lo, hi):
        sel = [slice(None)] * 3
        sel[axis] = position
        return u_ref.at[(pl.ds(lo, hi - lo),) + tuple(sel)]

    for colour in range(3):
        axis = ORDERS[colour][0]
        ends = (UNIT_LO[colour], UNIT_MID[colour], UNIT_HI[colour])
        far = peer_coord(axis, 2)
        for side, step in enumerate(RING):
            peer, near = peer_id(axis, step), peer_coord(axis, step)
            lo, hi = ends[side], ends[side + 1]
            pending[colour, side, 'stats'] = send(st_ref.at[pl.ds(colour, 2)], q1.at[colour, side], peer)
            pending[colour, side, 'relay'] = send(block(axis, far, lo, hi), relay.at[pl.ds(lo, hi - lo)], peer)
            lo, hi = ends[1 - side], ends[2 - side]
            pending[colour, side, 'near'] = send(block(axis, near, lo, hi), r1.at[0, pl.ds(lo, hi - lo)], peer)

    def ring_sum(colour, lo, hi, position, factors, arrays, store):
        axis = ORDERS[colour][0]
        first, second = [a for a in range(3) if a != axis]
        for i in range(4):
            for j in range(4):
                where = HEAD_STRIDE[first] * i + HEAD_STRIDE[second] * j
                at = [None] * 3
                at[axis], at[first], at[second] = position, i, j
                for bt in range(lo // 4, (hi - 1) // 4 + 1):
                    fb = [spread(f[bt - colour], where) for f in factors]
                    for unit in range(max(lo, bt * 4), min(hi, bt * 4 + 4)):
                        total = fb[0] * u_ref[unit, at[0], at[1], at[2]]
                        for f, array in zip(fb[1:], arrays):
                            total = total + f * array[unit, i, j]
                        store[unit, i, j] = total

    for colour in range(3):
        axis = ORDERS[colour][0]
        ends = (UNIT_LO[colour], UNIT_MID[colour], UNIT_HI[colour])
        for side, step in enumerate(RING):
            pending[colour, side, 'stats'].wait_recv()
            lo, hi = ends[side], ends[side + 1]
            peer, near = peer_id(axis, step), peer_coord(axis, step)
            pending[colour, side, 'relay'].wait_recv()
            merged, factors = merge_stats([st_ref[pl.ds(colour, 2)], q1[colour, side]], near * HEAD_STRIDE[axis], False)
            q0[colour, side] = merged
            ring_sum(colour, lo, hi, near, factors, [relay], passed)
            pending[colour, side, 'sum stats'] = send(q0.at[colour, side], q1.at[colour, 2 + side], peer)
            pending[colour, side, 'sum'] = send(passed.at[pl.ds(lo, hi - lo)], r1.at[1, pl.ds(lo, hi - lo)], peer)

    load_uv.wait()
    pick = lax.broadcasted_iota(jnp.int32, (64, 8, 128), 1) == lax.rem(head, 8)

    def pick_rows(i, carry):
        rows = pl.ds(pl.multiple_of(i * 64, 64), 64)
        wuv_h[rows, :] = jnp.sum(jnp.where(pick, wuv_v[rows].astype(f32), 0.0), axis=1).astype(bf16)
        return carry

    lax.fori_loop(0, 8, pick_rows, 0)

    for colour in range(3):
        order = ORDERS[colour]
        axis, axis2 = order[:2]
        lo, hi = UNIT_LO[colour], UNIT_HI[colour]
        ends = (lo, UNIT_MID[colour], hi)
        first, second = [a for a in range(3) if a != axis]
        for side in range(2):
            pending[colour, 1 - side, 'near'].wait_recv()
            pending[colour, side, 'sum stats'].wait_recv()
            pending[colour, side, 'sum'].wait_recv()
            stats = [st_ref[pl.ds(colour, 2)], q1[colour, 1 - side], q1[colour, 2 + side]]
            merged, factors = merge_stats(stats, coord[axis] * HEAD_STRIDE[axis])
            ring_sum(colour, ends[side], ends[side + 1], coord[axis], factors, [r1.at[0], r1.at[1]], v1)
        s1[colour] = merged
        for step in SEND_ORDER:
            pc = peer_coord(axis2, step)
            sel = (pc, slice(None)) if axis2 == first else (slice(None), pc)
            a = send(v1.at[(pl.ds(lo, hi - lo),) + sel], r2.at[step - 1, pl.ds(lo, hi - lo)], peer_id(axis2, step))
            b = send(s1.at[colour], q2.at[colour, step - 1], peer_id(axis2, step))
            pending[colour, step] = (a, b)

    for colour in range(3):
        order = ORDERS[colour]
        axis, axis2, axis3 = order
        lo, hi = UNIT_LO[colour], UNIT_HI[colour]
        first, second = [a for a in range(3) if a != axis]
        for step in WAIT_ORDER:
            for copy in pending[colour, step]:
                copy.wait_recv()
        stats = [s1[colour]] + [q2[colour, i] for i in range(3)]
        merged, factors = merge_stats(stats, coord[axis2] * HEAD_STRIDE[axis2])
        s2[colour] = merged
        for i in range(4):
            at = (coord[axis2], i) if axis2 == first else (i, coord[axis2])
            for bt in range(lo // 4, (hi - 1) // 4 + 1):
                fb = [spread(f[bt - colour], HEAD_STRIDE[axis3] * i) for f in factors]
                for unit in range(max(lo, bt * 4), min(hi, bt * 4 + 4)):
                    total = fb[0] * v1[unit, at[0], at[1]]
                    for k in range(3):
                        total = total + fb[k + 1] * r2[k, unit, i]
                    v2[unit, i] = total
        for step in SEND_ORDER:
            a = send(v2.at[pl.ds(lo, hi - lo), peer_coord(axis3, step)], r3.at[step - 1, pl.ds(lo, hi - lo)], peer_id(axis3, step))
            b = send(s2.at[colour], q3.at[colour, step - 1], peer_id(axis3, step))
            pending[colour, step] = (a, b)

    units = [None] * 16
    den = [None] * 16
    for colour in range(3):
        axis3 = ORDERS[colour][2]
        lo, hi = UNIT_LO[colour], UNIT_HI[colour]
        for step in WAIT_ORDER:
            for copy in pending[colour, step]:
                copy.wait_recv()
        stats = [s2[colour]] + [q3[colour, i] for i in range(3)]
        merged, factors = merge_stats(stats, coord[axis3] * HEAD_STRIDE[axis3])
        for bt in range(lo // 4, (hi - 1) // 4 + 1):
            fb = [spread(f[bt - colour], 0) for f in factors]
            dn = spread(merged[bt - colour], 64)
            for unit in range(max(lo, bt * 4), min(hi, bt * 4 + 4)):
                total = fb[0] * v2[unit, coord[axis3]]
                for k in range(3):
                    total = total + fb[k + 1] * r3[k, unit]
                units[unit] = total / dn
    o_lat = jnp.concatenate(
        [jnp.concatenate([units[bt * 4 + kt] for kt in range(4)], axis=1) for bt in range(4)], axis=0).astype(jnp.bfloat16)
    o_head = jnp.dot(o_lat, wuv_h[...], preferred_element_type=jnp.float32).astype(jnp.bfloat16)
    load_out.wait()
    for half in range(2):
        for cg in range(4):
            base = half * 2560 + cg * 640
            part = jnp.dot(o_head, wout_v[:, base:base + 640], preferred_element_type=jnp.float32)
            y_buf[half, :, cg] = part.reshape(4, 8, 640)

    pair = send(y_buf.at[1 - tp], y_in, {'tp': 1 - tp})
    pair.wait_recv()
    y_in[...] = y_in[...] + y_buf[tp]

    for colour in range(2):
        cols = pl.ds(OUT_LO[colour], OUT_HI[colour] - OUT_LO[colour])
        axis = colour
        for step in SEND_ORDER:
            pc = peer_coord(axis, step)
            src = y_in.at[pc, :, :, cols] if axis == 0 else y_in.at[:, pc, :, cols]
            pending[colour, step] = send(src, t1.at[step - 1, :, :, cols], peer_id(axis, step))
    for colour in range(2):
        cols = pl.ds(OUT_LO[colour], OUT_HI[colour] - OUT_LO[colour])
        axis, axis2 = colour, 1 - colour
        for step in WAIT_ORDER:
            pending[colour, step].wait_recv()
        for i in range(4):
            own = y_in[x, i, :, cols] if axis == 0 else y_in[i, y, :, cols]
            p1[i, :, cols] = own + sum(t1[k, i, :, cols] for k in range(3))
        for step in SEND_ORDER:
            pending[colour, step] = send(
                p1.at[peer_coord(axis2, step), :, cols], t2.at[step - 1, :, cols], peer_id(axis2, step))
    for colour in range(2):
        cols = pl.ds(OUT_LO[colour], OUT_HI[colour] - OUT_LO[colour])
        axis2 = 1 - colour
        for step in WAIT_ORDER:
            pending[colour, step].wait_recv()
        p2[:, cols] = p1[coord[axis2], :, cols] + sum(t2[k, :, cols] for k in range(3))

    for step in SEND_ORDER:
        pending[0, step] = send(p2, zbuf.at[z], peer_id(2, step))
    zbuf[z] = p2[...]
    for step in WAIT_ORDER:
        pending[0, step].wait_recv()
    g_buf[tp, x, y] = (zbuf[0] + zbuf[1]) + (zbuf[2] + zbuf[3])

    for colour in range(2):
        cols = pl.ds(OUT_LO[colour], OUT_HI[colour] - OUT_LO[colour])
        axis2 = 1 - colour
        mine = g_buf.at[tp, x, y, :, cols]
        for step in SEND_ORDER:
            pending[colour, step] = send(mine, mine, peer_id(axis2, step))
    for colour in range(2):
        cols = pl.ds(OUT_LO[colour], OUT_HI[colour] - OUT_LO[colour])
        axis = colour
        for step in WAIT_ORDER:
            pending[colour, step].wait_recv()
        mine = g_buf.at[tp, x, :, :, cols] if axis == 0 else g_buf.at[tp, :, y, :, cols]
        for step in SEND_ORDER:
            pending[colour, step] = send(mine, mine, peer_id(axis, step))
    for colour in range(2):
        for step in WAIT_ORDER:
            pending[colour, step].wait_recv()
    pair = send(g_buf.at[tp], g_buf.at[tp], {'tp': 1 - tp})
    pair.wait_recv()
    for half in range(2):
        for cg in range(4):
            base = half * 2560 + cg * 640
            out_ref[:, base:base + 640] = g_buf[half, :, cg].reshape(32, 640)
    for copy in started:
        copy.wait_send()


N_SENDS = 95


def tail(u_parts, stats, w_uv, w_out):
    parts = u_parts.shape[:3]
    cols = (8, 640)
    grid = parts[1:]
    vmem = pl.BlockSpec(memory_space=pltpu.VMEM)
    hbm = pl.BlockSpec(memory_space=pltpu.HBM)
    return pl.pallas_call(
        tail_kernel,
        out_shape=jax.ShapeDtypeStruct((32, 5120), f32),
        in_specs=[vmem, vmem, hbm, hbm],
        out_specs=vmem,
        scratch_shapes=[
            pltpu.VMEM(parts + TILE, f32),
            pltpu.VMEM(parts + TILE, f32),
            pltpu.VMEM((2,) + parts + TILE, f32),
            pltpu.VMEM(parts + TILE, f32),
            pltpu.VMEM((3,) + parts[:2] + TILE, f32),
            pltpu.VMEM(parts[:2] + TILE, f32),
            pltpu.VMEM((3,) + parts[:1] + TILE, f32),
            pltpu.VMEM((3, 2) + TILE, f32),
            pltpu.VMEM((3, 2) + TILE, f32),
            pltpu.VMEM((3, 2, 2) + TILE, f32),
            pltpu.VMEM((3, 4, 2) + TILE, f32),
            pltpu.VMEM((3, 3, 2) + TILE, f32),
            pltpu.VMEM((3, 3, 2) + TILE, f32),
            pltpu.VMEM((512,) + TILE, bf16),
            pltpu.VMEM((512, 128), bf16),
            pltpu.VMEM((128, 5120), bf16),
            pltpu.VMEM((2,) + grid + cols, f32),
            pltpu.VMEM(grid + cols, f32),
            pltpu.VMEM((3, 4) + cols, f32),
            pltpu.VMEM((3,) + cols, f32),
            pltpu.VMEM((4,) + cols, f32),
            pltpu.VMEM(cols, f32),
            pltpu.VMEM((4,) + cols, f32),
            pltpu.VMEM((2,) + grid + cols, f32),
            pltpu.SemaphoreType.DMA((N_SENDS,)),
            pltpu.SemaphoreType.DMA((N_SENDS,)),
            pltpu.SemaphoreType.DMA((2,)),
        ],
        compiler_params=pltpu.CompilerParams(collective_id=0, has_side_effects=True, vmem_limit_bytes=TAIL_VMEM),
        name='tail',
    )(u_parts, stats, w_uv, w_out)


def solution(mesh):
    row_spec = P('dp', None)
    cache_spec = P('dp', 'sp', None)
    head_spec = P(None, 'tp', None)
    in_specs = (row_spec, cache_spec, cache_spec, P('dp'), P(), P(), P(), P(), head_spec, head_spec, head_spec, P('tp', None))
    out_specs = (row_spec, cache_spec, cache_spec)

    def local_step(hidden, lat_cache, rope_cache, positions, w_dq, gain_q, w_dkv, gain_kv, w_uq, w_uk, w_uv, w_out):
        seq_local = lat_cache.shape[1]
        score_scale = YARN_MSCALE ** 2 / math.sqrt(w_uq.shape[2])
        cos_t, sin_t = rope_tables(positions, rope_cache.shape[2])
        q_abs, q_rope, lat_new, rope_new = front(hidden, gain_q, gain_kv, cos_t, sin_t, w_dkv, w_dq, w_uk, w_uq)
        base = (lax.axis_index('sp') * seq_local).reshape(1)
        lat_all, rope_all, u_parts, stats = attend(
            base, positions, q_abs, q_rope, lat_cache, rope_cache.transpose(0, 2, 1), lat_new, rope_new, score_scale)
        u_parts = u_parts.reshape(16, 4, 4, 4, 8, 128)
        attn_out = tail(u_parts, stats, w_uv, w_out)
        out = (hidden.astype(f32) + attn_out).astype(bf16)
        return out, lat_all, rope_all.transpose(0, 2, 1)

    return jax.shard_map(local_step, mesh=mesh, in_specs=in_specs, out_specs=out_specs, check_vma=False)
```

```python
import functools
import math
import jax
import jax.numpy as jnp
from jax import lax
from jax.experimental import pallas as pl
from jax.experimental.pallas import tpu as pltpu
from jax.sharding import PartitionSpec as P

EPSILON = 1e-6
ROPE_BASE = 50000.0
YARN_MSCALE = 1.0 + 0.1 * math.log(32.0)
MASK_VALUE = -1e30
TILE = (8, 128)
HEAD_GROUP = 16
UQ_RING = 4
MIB = 2 ** 20
FRONT_VMEM = 48 * MIB
ATTEND_VMEM = 46 * MIB
TAIL_VMEM = 48 * MIB
SEND_ORDER = (2, 1, 3)
WAIT_ORDER = (1, 3, 2)
MESH = pl.DeviceIdType.MESH
NT = (((1,), (1,)), ((), ()))
f32, bf16 = jnp.float32, jnp.bfloat16

HEAD_STRIDE = (16, 4, 1)
SP_STRIDE = (1, 4, 16)
ORDERS = ((0, 1, 2), (1, 2, 0), (2, 0, 1))
UNIT_LO = (0, 5, 10)
UNIT_MID = (2, 8, 13)
UNIT_HI = (5, 10, 16)
RING = (1, 3)
RING_STEPS = (1, 2, 3)
OUT_LO = (0, 256)
OUT_HI = (256, 640)


def rope_tables(positions, rope_dim):
    half_dim = rope_dim // 2
    inv_freq = ROPE_BASE ** (-jnp.arange(half_dim).astype(jnp.float32) / half_dim)
    angles = positions.astype(jnp.float32)[:, None] * inv_freq[None, :]
    return jnp.cos(angles), jnp.sin(angles)


def front_kernel(hid_ref, gq_ref, gkv_ref, cos_ref, sin_ref, wdkv_hbm, wdq_hbm, wuk_hbm, wuq_hbm,
                 qabs_ref, qrope_ref, lnew_ref, rnew_ref, wdkv_v, wdq_v, wuk_v, wuq_v, wk_v, nope_v, turn_v, ab_v, sem_kv, sem_q, sem_k, sem_u):
    n_kv, n_q, ring = wdkv_v.shape[0], wdq_v.shape[0], wuq_v.shape[0]
    kv_cols, q_rows, part = wdkv_v.shape[2], wdq_v.shape[1], wuq_v.shape[1]
    n_parts = wuq_hbm.shape[0] // part

    def load_uq(i):
        return pltpu.make_async_copy(wuq_hbm.at[pl.ds(i * part, part)], wuq_v.at[i % ring], sem_u.at[i % ring])

    kv_loads = [pltpu.make_async_copy(wdkv_hbm.at[:, pl.ds(i * kv_cols, kv_cols)], wdkv_v.at[i], sem_kv.at[i]) for i in range(n_kv)]
    q_loads = [pltpu.make_async_copy(wdq_hbm.at[pl.ds(i * q_rows, q_rows), :], wdq_v.at[i], sem_q.at[i]) for i in range(n_q)]
    k_rows = wuk_v.shape[0] // 4
    k_loads = [pltpu.make_async_copy(wuk_hbm.at[pl.ds(i * k_rows, k_rows)], wuk_v.at[pl.ds(i * k_rows, k_rows)], sem_k.at[i]) for i in range(4)]
    uq_loads = [load_uq(i) for i in range(n_parts)]
    queue = k_loads + kv_loads + q_loads + uq_loads
    state = [0]

    def issue(count):
        for copy in queue[state[0]:state[0] + count]:
            copy.start()
        state[0] += count

    issue(UQ_RING)
    cos_t, sin_t = cos_ref[...], sin_ref[...]
    half = cos_t.shape[1]

    def rotate(v):
        v1, v2 = v[:, :half], v[:, half:]
        return jnp.concatenate([v1 * cos_t - v2 * sin_t, v2 * cos_t + v1 * sin_t], axis=1)

    def norm(values, gain_ref):
        v = values.astype(bf16).astype(f32)
        inv = lax.rsqrt(jnp.mean(v * v, axis=1, keepdims=True) + EPSILON)
        return (v * inv * gain_ref[...].astype(f32)[None, :]).astype(bf16)

    for copy in k_loads:
        copy.wait()
        issue(1)
    kv = jnp.zeros((32, wdkv_v.shape[1]), f32)
    for i in range(n_kv):
        kv_loads[i].wait()
        issue(1)
        kv = kv + lax.dot_general(hid_ref[:, i * kv_cols:(i + 1) * kv_cols], wdkv_v[i], NT, preferred_element_type=f32)
    lnew_ref[...] = norm(kv[:, :512], gkv_ref)
    turned = rotate(kv[:, 512:].astype(bf16).astype(f32)).T.astype(bf16)
    for t in range(4):
        rnew_ref[t] = turned[:, t * 8:t * 8 + 8]
    h_q = jnp.zeros((32, 1536), f32)
    for i in range(n_q):
        q_loads[i].wait()
        issue(1)
        h_q = h_q + jnp.dot(hid_ref[:, i * q_rows:(i + 1) * q_rows], wdq_v[i], preferred_element_type=f32)
    cq = norm(h_q, gq_ref)

    zero = jnp.zeros((32, 128), bf16)
    per_group = HEAD_GROUP // part
    for i in range(n_parts):
        heads = slice(i // per_group * HEAD_GROUP, (i // per_group + 1) * HEAD_GROUP)
        first = i % per_group * part
        if first == 0:
            wk_v[...] = jnp.swapaxes(wuk_v[:, heads, :], 0, 1)
        uq_loads[i].wait()
        w = wuq_v[i % ring].reshape(part * 192, 1536)
        q4 = lax.dot_general(cq, w, NT, preferred_element_type=f32).astype(bf16)
        issue(1)
        for j in range(part):
            q = q4[:, j * 192:j * 192 + 192]
            nope_v[first + j] = q[:, :128]
            turn_v[first + j] = rotate(q[:, 128:].astype(f32))
        for j in range(first, first + part, 2):
            k = j + 1
            pair = jnp.concatenate([jnp.concatenate([nope_v[j], zero], axis=1), jnp.concatenate([zero, nope_v[k]], axis=1)], axis=0)
            both = lax.dot_general(pair, jnp.concatenate([wk_v[j], wk_v[k]], axis=1), NT, preferred_element_type=f32)
            ab_v[j], ab_v[k] = both[:32], both[32:]
        if first + part == HEAD_GROUP:
            qabs_ref[:, heads, :] = jnp.swapaxes(ab_v[...], 0, 1).astype(bf16)
            qrope_ref[:, heads, :] = jnp.swapaxes(turn_v[...], 0, 1).astype(bf16)


def front(hidden, gain_q, gain_kv, cos_t, sin_t, w_dkv, w_dq, w_uk, w_uq):
    heads = w_uq.shape[1]
    vmem = pl.BlockSpec(memory_space=pltpu.VMEM)
    hbm = pl.BlockSpec(memory_space=pltpu.HBM)
    dma = pltpu.SemaphoreType.DMA
    shape = jax.ShapeDtypeStruct
    return pl.pallas_call(
        front_kernel,
        out_shape=(shape((32, heads, 512), bf16), shape((32, heads, 64), bf16), shape((32, 512), bf16), shape((4, 64, 8), bf16)),
        in_specs=[vmem] * 5 + [hbm] * 4,
        out_specs=[vmem] * 4,
        scratch_shapes=[
            pltpu.VMEM((UQ_RING, 576, 1280), bf16),
            pltpu.VMEM((5, 1024, 1536), bf16),
            pltpu.VMEM((512, heads, 128), bf16),
            pltpu.VMEM((UQ_RING, 4, 192, 1536), bf16),
            pltpu.VMEM((HEAD_GROUP, 512, 128), bf16),
            pltpu.VMEM((HEAD_GROUP, 32, 128), bf16),
            pltpu.VMEM((HEAD_GROUP, 32, 64), f32),
            pltpu.VMEM((HEAD_GROUP, 32, 512), f32),
            dma((UQ_RING,)), dma((5,)), dma((UQ_RING,)), dma((UQ_RING,)),
        ],
        compiler_params=pltpu.CompilerParams(vmem_limit_bytes=FRONT_VMEM),
        name='front',
    )(hidden, gain_q, gain_kv, cos_t, sin_t, w_dkv.T, w_dq, w_uk, w_uq.transpose(1, 2, 0))


def attend_kernel(base_ref, pos_ref, qabs_ref, qrope_ref, lat_ref, rope_ref, lnew_ref, rnew_ref,
                  lat_out, rope_out, u_ref, st_ref, s_buf, w_buf, *, scale):
    tile = pl.program_id(0)
    base = base_ref[0]
    lane256 = lax.broadcasted_iota(jnp.int32, (64, 256), 1)
    lane128 = lax.broadcasted_iota(jnp.int32, (64, 128), 1)
    row16 = lax.broadcasted_iota(jnp.int32, (16, 512), 0)
    lat_out[...] = lat_ref[...]
    slots = [pos_ref[tile * 8 + b] - base for b in range(8)]
    for b in range(8):
        slot = slots[b]
        group = jnp.clip(slot // 16, 0, 15) * 16
        rows = pl.ds(pl.multiple_of(group, 16), 16)
        new = jnp.broadcast_to(lnew_ref[b:b + 1, :].astype(f32), (16, 512))
        lat_out[b, rows, :] = jnp.where(row16 == slot - group, new, lat_ref[b, rows, :].astype(f32)).astype(bf16)
        rope_out[b] = jnp.where(lane256 == slot, rnew_ref[0, :, b:b + 1].astype(f32), rope_ref[b].astype(f32)).astype(bf16)
    for b in range(8):
        s = lax.dot_general(qabs_ref[tile * 8 + b], lat_out[b], NT, preferred_element_type=f32)
        s_buf[b] = s + jnp.dot(qrope_ref[tile * 8 + b], rope_out[b], preferred_element_type=f32)
    tops = jnp.zeros((64, 128), f32)
    dens = jnp.zeros((64, 128), f32)
    for b in range(8):
        s = jnp.where(lane256 <= slots[b], s_buf[b] * scale, MASK_VALUE)
        top = jnp.max(s, axis=1, keepdims=True)
        w = jnp.exp(s - top)
        den = jnp.sum(w, axis=1, keepdims=True)
        w_buf[b] = w.astype(bf16)
        tops = jnp.where(lane128 == b, top, tops)
        dens = jnp.where(lane128 == b, den, dens)
    st_ref[0] = jnp.concatenate([tops, dens], axis=0).T[:8, :]
    for b in range(8):
        u = jnp.dot(w_buf[b], lat_out[b], preferred_element_type=f32)
        for kt in range(4):
            u_ref[tile * 4 + kt, pl.ds(b, 64, stride=8), :] = u[:, kt * 128:kt * 128 + 128]


def attend(base, positions, q_abs, q_rope, lat_cache, rope_t, lat_new, rope_new, scale):
    vmem = pl.BlockSpec(memory_space=pltpu.VMEM)
    smem = pl.BlockSpec(memory_space=pltpu.SMEM)
    first = lambda t: (t, 0, 0)
    return pl.pallas_call(
        functools.partial(attend_kernel, scale=scale),
        grid=(4,),
        out_shape=(jax.ShapeDtypeStruct((32, 256, 512), bf16), jax.ShapeDtypeStruct((32, 64, 256), bf16),
                   jax.ShapeDtypeStruct((16, 512, 128), f32), jax.ShapeDtypeStruct((4, 8, 128), f32)),
        in_specs=[smem, smem,
                  vmem, vmem,
                  pl.BlockSpec((8, 256, 512), first), pl.BlockSpec((8, 64, 256), first),
                  pl.BlockSpec((8, 512), lambda t: (t, 0)), pl.BlockSpec((1, 64, 8), first)],
        out_specs=[pl.BlockSpec((8, 256, 512), first), pl.BlockSpec((8, 64, 256), first),
                   vmem, pl.BlockSpec((1, 8, 128), first)],
        scratch_shapes=[pltpu.VMEM((8, 64, 256), f32), pltpu.VMEM((8, 64, 256), bf16)],
        compiler_params=pltpu.CompilerParams(vmem_limit_bytes=ATTEND_VMEM),
        name='attend',
    )(base, positions, q_abs, q_rope, lat_cache, rope_t, lat_new, rope_new)


def tail_kernel(u_ref, st_ref, wuv_ref, wout_ref, out_ref,
                relay, passed, r1, v1, r2, v2, r3, s1, s2, q0, q1, q2, q3,
                wuv_v, wuv_h, wout_v, y_buf, y_in, t1, t2, p1, p2, zbuf, g_buf,
                send_sem, recv_sem, load_sem):
    sp = lax.axis_index('sp')
    tp = lax.axis_index('tp')
    coord = (lax.rem(sp, 4), lax.rem(sp // 4, 4), sp // 16)
    x, y, z = coord
    head = x * 16 + y * 4 + z
    group = pl.multiple_of((head // 8) * 8, 8)

    load_uv = pltpu.make_async_copy(wuv_ref.at[:, pl.ds(group, 8), :], wuv_v, load_sem.at[0])
    load_uv.start()
    load_out = pltpu.make_async_copy(wout_ref.at[pl.ds(pl.multiple_of(head * 128, 128), 128), :], wout_v, load_sem.at[1])
    load_out.start()

    def peer_coord(axis, step):
        return lax.rem(coord[axis] + step, 4)

    def peer_id(axis, step):
        return {'sp': sp + (peer_coord(axis, step) - coord[axis]) * SP_STRIDE[axis]}

    barrier = pltpu.get_barrier_semaphore()
    for axis in range(3):
        for step in RING_STEPS:
            pl.semaphore_signal(barrier, inc=1, device_id=peer_id(axis, step), device_id_type=MESH)
    pl.semaphore_signal(barrier, inc=1, device_id={'tp': 1 - tp}, device_id_type=MESH)
    pl.semaphore_wait(barrier, 10)

    started = []

    def send(src, dst, device):
        index = len(started)
        copy = pltpu.make_async_remote_copy(
            src_ref=src, dst_ref=dst, send_sem=send_sem.at[index], recv_sem=recv_sem.at[index],
            device_id=device, device_id_type=MESH)
        copy.start()
        started.append(copy)
        return copy

    lane = lax.broadcasted_iota(jnp.int32, (2, 8, 128), 2)

    def merge_stats(stats, offset, turn_result=True):
        top = functools.reduce(jnp.maximum, stats)
        shift = lax.rem(128 - offset, 128)
        factors = [jnp.exp(s - top) for s in stats]
        den = sum(f * pltpu.roll(s, 64, 2) for f, s in zip(factors, stats))
        merged = jnp.where(lane < 64, top, pltpu.roll(den, 64, 2))
        if turn_result:
            merged = pltpu.roll(merged, shift, 2)
        return merged, [pltpu.roll(f, shift, 2) for f in factors]

    def spread(factor, lane_index):
        return jnp.broadcast_to(factor[:, lane_index:lane_index + 1], (8, 128))

    pending = {}

    def block(axis, position, lo, hi):
        sel = [slice(None)] * 3
        sel[axis] = position
        return u_ref.at[(pl.ds(lo, hi - lo),) + tuple(sel)]

    for colour in range(3):
        axis = ORDERS[colour][0]
        ends = (UNIT_LO[colour], UNIT_MID[colour], UNIT_HI[colour])
        far = peer_coord(axis, 2)
        for side, step in enumerate(RING):
            peer, near = peer_id(axis, step), peer_coord(axis, step)
            lo, hi = ends[side], ends[side + 1]
            pending[colour, side, 'stats'] = send(st_ref.at[pl.ds(colour, 2)], q1.at[colour, side], peer)
            pending[colour, side, 'relay'] = send(block(axis, far, lo, hi), relay.at[pl.ds(lo, hi - lo)], peer)
            lo, hi = ends[1 - side], ends[2 - side]
            pending[colour, side, 'near'] = send(block(axis, near, lo, hi), r1.at[0, pl.ds(lo, hi - lo)], peer)

    def ring_sum(colour, lo, hi, position, factors, arrays, store):
        axis = ORDERS[colour][0]
        first, second = [a for a in range(3) if a != axis]
        for i in range(4):
            for j in range(4):
                where = HEAD_STRIDE[first] * i + HEAD_STRIDE[second] * j
                at = [None] * 3
                at[axis], at[first], at[second] = position, i, j
                for bt in range(lo // 4, (hi - 1) // 4 + 1):
                    fb = [spread(f[bt - colour], where) for f in factors]
                    for unit in range(max(lo, bt * 4), min(hi, bt * 4 + 4)):
                        total = fb[0] * u_ref[unit, at[0], at[1], at[2]]
                        for f, array in zip(fb[1:], arrays):
                            total = total + f * array[unit, i, j]
                        store[unit, i, j] = total

    for colour in range(3):
        axis = ORDERS[colour][0]
        ends = (UNIT_LO[colour], UNIT_MID[colour], UNIT_HI[colour])
        for side, step in enumerate(RING):
            pending[colour, side, 'stats'].wait_recv()
            lo, hi = ends[side], ends[side + 1]
            peer, near = peer_id(axis, step), peer_coord(axis, step)
            pending[colour, side, 'relay'].wait_recv()
            merged, factors = merge_stats([st_ref[pl.ds(colour, 2)], q1[colour, side]], near * HEAD_STRIDE[axis], False)
            q0[colour, side] = merged
            ring_sum(colour, lo, hi, near, factors, [relay], passed)
            pending[colour, side, 'sum stats'] = send(q0.at[colour, side], q1.at[colour, 2 + side], peer)
            pending[colour, side, 'sum'] = send(passed.at[pl.ds(lo, hi - lo)], r1.at[1, pl.ds(lo, hi - lo)], peer)

    load_uv.wait()
    pick = lax.broadcasted_iota(jnp.int32, (64, 8, 128), 1) == lax.rem(head, 8)

    def pick_rows(i, carry):
        rows = pl.ds(pl.multiple_of(i * 64, 64), 64)
        wuv_h[rows, :] = jnp.sum(jnp.where(pick, wuv_v[rows].astype(f32), 0.0), axis=1).astype(bf16)
        return carry

    lax.fori_loop(0, 8, pick_rows, 0)

    for colour in range(3):
        order = ORDERS[colour]
        axis, axis2 = order[:2]
        lo, hi = UNIT_LO[colour], UNIT_HI[colour]
        ends = (lo, UNIT_MID[colour], hi)
        first, second = [a for a in range(3) if a != axis]
        for side in range(2):
            pending[colour, 1 - side, 'near'].wait_recv()
            pending[colour, side, 'sum stats'].wait_recv()
            pending[colour, side, 'sum'].wait_recv()
            stats = [st_ref[pl.ds(colour, 2)], q1[colour, 1 - side], q1[colour, 2 + side]]
            merged, factors = merge_stats(stats, coord[axis] * HEAD_STRIDE[axis])
            ring_sum(colour, ends[side], ends[side + 1], coord[axis], factors, [r1.at[0], r1.at[1]], v1)
        s1[colour] = merged
        for step in SEND_ORDER:
            pc = peer_coord(axis2, step)
            sel = (pc, slice(None)) if axis2 == first else (slice(None), pc)
            a = send(v1.at[(pl.ds(lo, hi - lo),) + sel], r2.at[step - 1, pl.ds(lo, hi - lo)], peer_id(axis2, step))
            b = send(s1.at[colour], q2.at[colour, step - 1], peer_id(axis2, step))
            pending[colour, step] = (a, b)

    for colour in range(3):
        order = ORDERS[colour]
        axis, axis2, axis3 = order
        lo, hi = UNIT_LO[colour], UNIT_HI[colour]
        first, second = [a for a in range(3) if a != axis]
        for step in WAIT_ORDER:
            for copy in pending[colour, step]:
                copy.wait_recv()
        stats = [s1[colour]] + [q2[colour, i] for i in range(3)]
        merged, factors = merge_stats(stats, coord[axis2] * HEAD_STRIDE[axis2])
        s2[colour] = merged
        for i in range(4):
            at = (coord[axis2], i) if axis2 == first else (i, coord[axis2])
            for bt in range(lo // 4, (hi - 1) // 4 + 1):
                fb = [spread(f[bt - colour], HEAD_STRIDE[axis3] * i) for f in factors]
                for unit in range(max(lo, bt * 4), min(hi, bt * 4 + 4)):
                    total = fb[0] * v1[unit, at[0], at[1]]
                    for k in range(3):
                        total = total + fb[k + 1] * r2[k, unit, i]
                    v2[unit, i] = total
        for step in SEND_ORDER:
            a = send(v2.at[pl.ds(lo, hi - lo), peer_coord(axis3, step)], r3.at[step - 1, pl.ds(lo, hi - lo)], peer_id(axis3, step))
            b = send(s2.at[colour], q3.at[colour, step - 1], peer_id(axis3, step))
            pending[colour, step] = (a, b)

    units = [None] * 16
    den = [None] * 16
    for colour in range(3):
        axis3 = ORDERS[colour][2]
        lo, hi = UNIT_LO[colour], UNIT_HI[colour]
        for step in WAIT_ORDER:
            for copy in pending[colour, step]:
                copy.wait_recv()
        stats = [s2[colour]] + [q3[colour, i] for i in range(3)]
        merged, factors = merge_stats(stats, coord[axis3] * HEAD_STRIDE[axis3])
        for bt in range(lo // 4, (hi - 1) // 4 + 1):
            fb = [spread(f[bt - colour], 0) for f in factors]
            dn = spread(merged[bt - colour], 64)
            for unit in range(max(lo, bt * 4), min(hi, bt * 4 + 4)):
                total = fb[0] * v2[unit, coord[axis3]]
                for k in range(3):
                    total = total + fb[k + 1] * r3[k, unit]
                units[unit] = total / dn
    o_lat = jnp.concatenate(
        [jnp.concatenate([units[bt * 4 + kt] for kt in range(4)], axis=1) for bt in range(4)], axis=0).astype(jnp.bfloat16)
    o_head = jnp.dot(o_lat, wuv_h[...], preferred_element_type=jnp.float32).astype(jnp.bfloat16)
    load_out.wait()
    def project(half):
        for cg in range(4):
            columns = pl.ds(pl.multiple_of((half * 4 + cg) * 640, 128), 640)
            part = jnp.dot(o_head, wout_v[:, columns], preferred_element_type=f32)
            y_buf[half, :, cg] = part.reshape(4, 8, 640)

    project(1 - tp)
    pair = send(y_buf.at[1 - tp], y_in, {'tp': 1 - tp})
    project(tp)
    pair.wait_recv()
    y_in[...] = y_in[...] + y_buf[tp]

    for colour in range(2):
        cols = pl.ds(OUT_LO[colour], OUT_HI[colour] - OUT_LO[colour])
        axis = colour
        for step in SEND_ORDER:
            pc = peer_coord(axis, step)
            src = y_in.at[pc, :, :, cols] if axis == 0 else y_in.at[:, pc, :, cols]
            pending[colour, step] = send(src, t1.at[step - 1, :, :, cols], peer_id(axis, step))
    for colour in range(2):
        cols = pl.ds(OUT_LO[colour], OUT_HI[colour] - OUT_LO[colour])
        axis, axis2 = colour, 1 - colour
        for step in WAIT_ORDER:
            pending[colour, step].wait_recv()
        for i in range(4):
            own = y_in[x, i, :, cols] if axis == 0 else y_in[i, y, :, cols]
            p1[i, :, cols] = own + sum(t1[k, i, :, cols] for k in range(3))
        for step in SEND_ORDER:
            pending[colour, step] = send(
                p1.at[peer_coord(axis2, step), :, cols], t2.at[step - 1, :, cols], peer_id(axis2, step))
    for colour in range(2):
        cols = pl.ds(OUT_LO[colour], OUT_HI[colour] - OUT_LO[colour])
        axis2 = 1 - colour
        for step in WAIT_ORDER:
            pending[colour, step].wait_recv()
        p2[:, cols] = p1[coord[axis2], :, cols] + sum(t2[k, :, cols] for k in range(3))

    for step in SEND_ORDER:
        pending[0, step] = send(p2, zbuf.at[z], peer_id(2, step))
    zbuf[z] = p2[...]
    for step in WAIT_ORDER:
        pending[0, step].wait_recv()
    g_buf[tp, x, y] = (zbuf[0] + zbuf[1]) + (zbuf[2] + zbuf[3])

    for colour in range(2):
        cols = pl.ds(OUT_LO[colour], OUT_HI[colour] - OUT_LO[colour])
        axis2 = 1 - colour
        mine = g_buf.at[tp, x, y, :, cols]
        for step in SEND_ORDER:
            pending[colour, step] = send(mine, mine, peer_id(axis2, step))
    for colour in range(2):
        cols = pl.ds(OUT_LO[colour], OUT_HI[colour] - OUT_LO[colour])
        axis = colour
        for step in WAIT_ORDER:
            pending[colour, step].wait_recv()
        mine = g_buf.at[tp, x, :, :, cols] if axis == 0 else g_buf.at[tp, :, y, :, cols]
        for step in SEND_ORDER:
            pending[colour, step] = send(mine, mine, peer_id(axis, step))
    pairs = []
    for colour in range(2):
        cols = pl.ds(OUT_LO[colour], OUT_HI[colour] - OUT_LO[colour])
        for step in WAIT_ORDER:
            pending[colour, step].wait_recv()
        mine = g_buf.at[tp, :, :, :, cols]
        pairs.append(send(mine, mine, {'tp': 1 - tp}))
    for pair in pairs:
        pair.wait_recv()
    for half in range(2):
        for cg in range(4):
            base = (half * 4 + cg) * 640
            out_ref[:, base:base + 640] = g_buf[half, :, cg].reshape(32, 640)
    for copy in started:
        copy.wait_send()


N_SENDS = 96


def tail(u_parts, stats, w_uv, w_out):
    parts = u_parts.shape[:3]
    cols = (8, 640)
    grid = parts[1:]
    vmem = pl.BlockSpec(memory_space=pltpu.VMEM)
    hbm = pl.BlockSpec(memory_space=pltpu.HBM)
    return pl.pallas_call(
        tail_kernel,
        out_shape=jax.ShapeDtypeStruct((32, 5120), f32),
        in_specs=[vmem, vmem, hbm, hbm],
        out_specs=vmem,
        scratch_shapes=[
            pltpu.VMEM(parts + TILE, f32),
            pltpu.VMEM(parts + TILE, f32),
            pltpu.VMEM((2,) + parts + TILE, f32),
            pltpu.VMEM(parts + TILE, f32),
            pltpu.VMEM((3,) + parts[:2] + TILE, f32),
            pltpu.VMEM(parts[:2] + TILE, f32),
            pltpu.VMEM((3,) + parts[:1] + TILE, f32),
            pltpu.VMEM((3, 2) + TILE, f32),
            pltpu.VMEM((3, 2) + TILE, f32),
            pltpu.VMEM((3, 2, 2) + TILE, f32),
            pltpu.VMEM((3, 4, 2) + TILE, f32),
            pltpu.VMEM((3, 3, 2) + TILE, f32),
            pltpu.VMEM((3, 3, 2) + TILE, f32),
            pltpu.VMEM((512,) + TILE, bf16),
            pltpu.VMEM((512, 128), bf16),
            pltpu.VMEM((128, 5120), bf16),
            pltpu.VMEM((2,) + grid + cols, f32),
            pltpu.VMEM(grid + cols, f32),
            pltpu.VMEM((3, 4) + cols, f32),
            pltpu.VMEM((3,) + cols, f32),
            pltpu.VMEM((4,) + cols, f32),
            pltpu.VMEM(cols, f32),
            pltpu.VMEM((4,) + cols, f32),
            pltpu.VMEM((2,) + grid + cols, f32),
            pltpu.SemaphoreType.DMA((N_SENDS,)),
            pltpu.SemaphoreType.DMA((N_SENDS,)),
            pltpu.SemaphoreType.DMA((2,)),
        ],
        compiler_params=pltpu.CompilerParams(collective_id=0, has_side_effects=True, vmem_limit_bytes=TAIL_VMEM),
        name='tail',
    )(u_parts, stats, w_uv, w_out)


def solution(mesh):
    row_spec = P('dp', None)
    cache_spec = P('dp', 'sp', None)
    head_spec = P(None, 'tp', None)
    in_specs = (row_spec, cache_spec, cache_spec, P('dp'), P(), P(), P(), P(), head_spec, head_spec, head_spec, P('tp', None))
    out_specs = (row_spec, cache_spec, cache_spec)

    def local_step(hidden, lat_cache, rope_cache, positions, w_dq, gain_q, w_dkv, gain_kv, w_uq, w_uk, w_uv, w_out):
        seq_local = lat_cache.shape[1]
        score_scale = YARN_MSCALE ** 2 / math.sqrt(w_uq.shape[2])
        cos_t, sin_t = rope_tables(positions, rope_cache.shape[2])
        q_abs, q_rope, lat_new, rope_new = front(hidden, gain_q, gain_kv, cos_t, sin_t, w_dkv, w_dq, w_uk, w_uq)
        base = (lax.axis_index('sp') * seq_local).reshape(1)
        lat_all, rope_all, u_parts, stats = attend(
            base, positions, q_abs, q_rope, lat_cache, rope_cache.transpose(0, 2, 1), lat_new, rope_new, score_scale)
        u_parts = u_parts.reshape(16, 4, 4, 4, 8, 128)
        attn_out = tail(u_parts, stats, w_uv, w_out)
        out = (hidden.astype(f32) + attn_out).astype(bf16)
        return out, lat_all, rope_all.transpose(0, 2, 1)

    return jax.shard_map(local_step, mesh=mesh, in_specs=in_specs, out_specs=out_specs, check_vma=False)
```

```python
import functools
import math
import jax
import jax.numpy as jnp
from jax import lax
from jax.experimental import pallas as pl
from jax.experimental.pallas import tpu as pltpu
from jax.sharding import PartitionSpec as P

EPSILON = 1e-6
ROPE_BASE = 50000.0
YARN_MSCALE = 1.0 + 0.1 * math.log(32.0)
MASK_VALUE = -1e30
TILE = (8, 128)
HEAD_GROUP = 16
UQ_RING = 4
MIB = 2 ** 20
FRONT_VMEM = 48 * MIB
ATTEND_VMEM = 46 * MIB
TAIL_VMEM = 48 * MIB
SEND_ORDER = (2, 1, 3)
WAIT_ORDER = (1, 3, 2)
MESH = pl.DeviceIdType.MESH
NT = (((1,), (1,)), ((), ()))
f32, bf16 = jnp.float32, jnp.bfloat16

HEAD_STRIDE = (16, 4, 1)
SP_STRIDE = (1, 4, 16)
ORDERS = ((0, 1, 2), (1, 2, 0), (2, 0, 1))
UNIT_LO = (0, 5, 10)
UNIT_MID = (2, 8, 13)
UNIT_HI = (5, 10, 16)
RING = (1, 3)
RING_STEPS = (1, 2, 3)
OUT_LO = (0, 256)
OUT_HI = (256, 640)


def rope_tables(positions, rope_dim):
    half_dim = rope_dim // 2
    inv_freq = ROPE_BASE ** (-jnp.arange(half_dim).astype(jnp.float32) / half_dim)
    angles = positions.astype(f32)[:, None] * inv_freq[None, :]
    return jnp.cos(angles), jnp.sin(angles)


def front_kernel(hid_ref, gain_ref, cos_ref, sin_ref, wdkv_hbm, wdq_hbm, wuk_hbm, wuq_hbm,
                 qabs_ref, qrope_ref, lnew_ref, rnew_ref, wdkv_v, wdq_v, wuk_v, wuq_v, wk_v, nope_v, turn_v, ab_v, sem_kv, sem_q, sem_k, sem_u):
    n_kv, n_q, ring = wdkv_v.shape[0], wdq_v.shape[0], wuq_v.shape[0]
    kv_cols, q_rows, part = wdkv_v.shape[2], wdq_v.shape[1], wuq_v.shape[1]
    n_parts = wuq_hbm.shape[0] // part

    def load_uq(i):
        return pltpu.make_async_copy(wuq_hbm.at[pl.ds(i * part, part)], wuq_v.at[i % ring], sem_u.at[i % ring])

    kv_loads = [pltpu.make_async_copy(wdkv_hbm.at[:, pl.ds(i * kv_cols, kv_cols)], wdkv_v.at[i], sem_kv.at[i]) for i in range(n_kv)]
    q_loads = [pltpu.make_async_copy(wdq_hbm.at[pl.ds(i * q_rows, q_rows), :], wdq_v.at[i], sem_q.at[i]) for i in range(n_q)]
    k_rows = wuk_v.shape[0] // 4
    k_loads = [pltpu.make_async_copy(wuk_hbm.at[pl.ds(i * k_rows, k_rows)], wuk_v.at[pl.ds(i * k_rows, k_rows)], sem_k.at[i]) for i in range(4)]
    uq_loads = [load_uq(i) for i in range(n_parts)]
    queue = kv_loads + q_loads + k_loads + uq_loads
    state = [0]

    def issue(count):
        for copy in queue[state[0]:state[0] + count]:
            copy.start()
        state[0] += count

    issue(UQ_RING)
    cos_t, sin_t = cos_ref[...], sin_ref[...]
    half = cos_t.shape[1]

    def rotate(v):
        v1, v2 = v[:, :half], v[:, half:]
        return jnp.concatenate([v1 * cos_t - v2 * sin_t, v2 * cos_t + v1 * sin_t], axis=1)

    def norm(values, gain):
        v = values.astype(bf16).astype(f32)
        inv = lax.rsqrt(jnp.mean(v * v, axis=1, keepdims=True) + EPSILON)
        return (v * inv * gain.astype(f32)[None, :]).astype(bf16)

    kv = jnp.zeros((32, wdkv_v.shape[1]), f32)
    for i in range(n_kv):
        kv_loads[i].wait()
        issue(1)
        kv = kv + lax.dot_general(hid_ref[:, i * kv_cols:(i + 1) * kv_cols], wdkv_v[i], NT, preferred_element_type=f32)
    lnew_ref[...] = norm(kv[:, :512], gain_ref[1536:])
    turned = rotate(kv[:, 512:].astype(bf16).astype(f32)).T.astype(bf16)
    for t in range(4):
        rnew_ref[t] = turned[:, t * 8:t * 8 + 8]
    h_q = jnp.zeros((32, 1536), f32)
    for i in range(n_q):
        q_loads[i].wait()
        issue(1)
        h_q = h_q + jnp.dot(hid_ref[:, i * q_rows:(i + 1) * q_rows], wdq_v[i], preferred_element_type=f32)
    cq = norm(h_q, gain_ref[:1536])
    for copy in k_loads:
        copy.wait()
        issue(1)

    zero = jnp.zeros((32, 128), bf16)
    per_group = HEAD_GROUP // part
    for i in range(n_parts):
        heads = slice(i // per_group * HEAD_GROUP, (i // per_group + 1) * HEAD_GROUP)
        first = i % per_group * part
        if first == 0:
            wk_v[...] = jnp.swapaxes(wuk_v[:, heads, :], 0, 1)
        uq_loads[i].wait()
        w = wuq_v[i % ring].reshape(part * 192, 1536)
        q4 = lax.dot_general(cq, w, NT, preferred_element_type=f32).astype(bf16)
        issue(1)
        for j in range(part):
            q = q4[:, j * 192:j * 192 + 192]
            nope_v[first + j] = q[:, :128]
            turn_v[first + j] = rotate(q[:, 128:].astype(f32))
        for j in range(first, first + part, 2):
            k = j + 1
            pair = jnp.concatenate([jnp.concatenate([nope_v[j], zero], axis=1), jnp.concatenate([zero, nope_v[k]], axis=1)], axis=0)
            both = lax.dot_general(pair, jnp.concatenate([wk_v[j], wk_v[k]], axis=1), NT, preferred_element_type=f32)
            ab_v[j], ab_v[k] = both[:32], both[32:]
        if first + part == HEAD_GROUP:
            qabs_ref[:, heads, :] = jnp.swapaxes(ab_v[...], 0, 1).astype(bf16)
            qrope_ref[:, heads, :] = jnp.swapaxes(turn_v[...], 0, 1).astype(bf16)


def front(hidden, gain_q, gain_kv, cos_t, sin_t, w_dkv, w_dq, w_uk, w_uq):
    heads = w_uq.shape[1]
    vmem = pl.BlockSpec(memory_space=pltpu.VMEM)
    hbm = pl.BlockSpec(memory_space=pltpu.HBM)
    dma = pltpu.SemaphoreType.DMA
    shape = jax.ShapeDtypeStruct
    return pl.pallas_call(
        front_kernel,
        out_shape=(shape((32, heads, 512), bf16), shape((32, heads, 64), bf16), shape((32, 512), bf16), shape((4, 64, 8), bf16)),
        in_specs=[vmem] * 4 + [hbm] * 4,
        out_specs=[vmem] * 4,
        scratch_shapes=[
            pltpu.VMEM((UQ_RING, 576, 1280), bf16),
            pltpu.VMEM((5, 1024, 1536), bf16),
            pltpu.VMEM((512, heads, 128), bf16),
            pltpu.VMEM((UQ_RING, 4, 192, 1536), bf16),
            pltpu.VMEM((HEAD_GROUP, 512, 128), bf16),
            pltpu.VMEM((HEAD_GROUP, 32, 128), bf16),
            pltpu.VMEM((HEAD_GROUP, 32, 64), f32),
            pltpu.VMEM((HEAD_GROUP, 32, 512), f32),
            dma((UQ_RING,)), dma((5,)), dma((UQ_RING,)), dma((UQ_RING,)),
        ],
        compiler_params=pltpu.CompilerParams(vmem_limit_bytes=FRONT_VMEM),
        name='front',
    )(hidden, jnp.concatenate([gain_q, gain_kv]), cos_t, sin_t, w_dkv.T, w_dq, w_uk, w_uq.transpose(1, 2, 0))


def attend_kernel(base_ref, pos_ref, qabs_ref, qrope_ref, lat_ref, rope_ref, lnew_ref, rnew_ref,
                  lat_out, rope_out, u_ref, st_ref, s_buf, w_buf, *, scale):
    tile = pl.program_id(0)
    base = base_ref[0]
    lane256 = lax.broadcasted_iota(jnp.int32, (64, 256), 1)
    lane128 = lax.broadcasted_iota(jnp.int32, (64, 128), 1)
    row16 = lax.broadcasted_iota(jnp.int32, (16, 512), 0)
    lat_out[...] = lat_ref[...]
    slots = [pos_ref[tile * 8 + b] - base for b in range(8)]
    for b in range(8):
        slot = slots[b]
        group = jnp.clip(slot // 16, 0, 15) * 16
        rows = pl.ds(pl.multiple_of(group, 16), 16)
        new = jnp.broadcast_to(lnew_ref[b:b + 1, :].astype(f32), (16, 512))
        lat_out[b, rows, :] = jnp.where(row16 == slot - group, new, lat_ref[b, rows, :].astype(f32)).astype(bf16)
        rope_out[b] = jnp.where(lane256 == slot, rnew_ref[0, :, b:b + 1].astype(f32), rope_ref[b].astype(f32)).astype(bf16)
    for b in range(8):
        s = lax.dot_general(qabs_ref[tile * 8 + b], lat_out[b], NT, preferred_element_type=f32)
        s_buf[b] = s + jnp.dot(qrope_ref[tile * 8 + b], rope_out[b], preferred_element_type=f32)
    tops = jnp.zeros((64, 128), f32)
    dens = jnp.zeros((64, 128), f32)
    for b in range(8):
        s = jnp.where(lane256 <= slots[b], s_buf[b] * scale, MASK_VALUE)
        top = jnp.max(s, axis=1, keepdims=True)
        w = jnp.exp(s - top)
        den = jnp.sum(w, axis=1, keepdims=True)
        w_buf[b] = w.astype(bf16)
        tops = jnp.where(lane128 == b, top, tops)
        dens = jnp.where(lane128 == b, den, dens)
    st_ref[0] = jnp.concatenate([tops, dens], axis=0).T[:8, :]
    for b in range(8):
        u = jnp.dot(w_buf[b], lat_out[b], preferred_element_type=f32)
        for kt in range(4):
            u_ref[tile * 4 + kt, pl.ds(b, 64, stride=8), :] = u[:, kt * 128:kt * 128 + 128]


def attend(base, positions, q_abs, q_rope, lat_cache, rope_t, lat_new, rope_new, scale):
    vmem = pl.BlockSpec(memory_space=pltpu.VMEM)
    smem = pl.BlockSpec(memory_space=pltpu.SMEM)
    first = lambda t: (t, 0, 0)
    return pl.pallas_call(
        functools.partial(attend_kernel, scale=scale),
        grid=(4,),
        out_shape=(jax.ShapeDtypeStruct((32, 256, 512), bf16), jax.ShapeDtypeStruct((32, 64, 256), bf16),
                   jax.ShapeDtypeStruct((16, 512, 128), f32), jax.ShapeDtypeStruct((4, 8, 128), f32)),
        in_specs=[smem, smem,
                  vmem, vmem,
                  pl.BlockSpec((8, 256, 512), first), pl.BlockSpec((8, 64, 256), first),
                  pl.BlockSpec((8, 512), lambda t: (t, 0)), pl.BlockSpec((1, 64, 8), first)],
        out_specs=[pl.BlockSpec((8, 256, 512), first), pl.BlockSpec((8, 64, 256), first),
                   vmem, pl.BlockSpec((1, 8, 128), first)],
        scratch_shapes=[pltpu.VMEM((8, 64, 256), f32), pltpu.VMEM((8, 64, 256), bf16)],
        compiler_params=pltpu.CompilerParams(vmem_limit_bytes=ATTEND_VMEM),
        name='attend',
    )(base, positions, q_abs, q_rope, lat_cache, rope_t, lat_new, rope_new)


def tail_kernel(u_ref, st_ref, wuv_ref, wout_ref, out_ref,
                relay, passed, r1, v1, r2, v2, r3, s1, s2, q0, q1, q2, q3,
                wuv_v, wuv_h, wout_v, y_buf, y_in, t1, t2, p1, p2, zbuf, g_buf,
                send_sem, recv_sem, load_sem):
    sp = lax.axis_index('sp')
    tp = lax.axis_index('tp')
    coord = (lax.rem(sp, 4), lax.rem(sp // 4, 4), sp // 16)
    x, y, z = coord
    head = x * 16 + y * 4 + z
    group = pl.multiple_of((head // 8) * 8, 8)

    load_uv = pltpu.make_async_copy(wuv_ref.at[:, pl.ds(group, 8), :], wuv_v, load_sem.at[0])
    load_uv.start()
    load_out = pltpu.make_async_copy(wout_ref.at[pl.ds(pl.multiple_of(head * 128, 128), 128), :], wout_v, load_sem.at[1])
    load_out.start()

    def peer_coord(axis, step):
        return lax.rem(coord[axis] + step, 4)

    def peer_id(axis, step):
        return {'sp': sp + (peer_coord(axis, step) - coord[axis]) * SP_STRIDE[axis]}

    barrier = pltpu.get_barrier_semaphore()
    for axis in range(3):
        for step in RING_STEPS:
            pl.semaphore_signal(barrier, inc=1, device_id=peer_id(axis, step), device_id_type=MESH)
    pl.semaphore_signal(barrier, inc=1, device_id={'tp': 1 - tp}, device_id_type=MESH)
    pl.semaphore_wait(barrier, 10)

    started = []

    def send(src, dst, device):
        index = len(started)
        copy = pltpu.make_async_remote_copy(
            src_ref=src, dst_ref=dst, send_sem=send_sem.at[index], recv_sem=recv_sem.at[index],
            device_id=device, device_id_type=MESH)
        copy.start()
        started.append(copy)
        return copy

    lane = lax.broadcasted_iota(jnp.int32, (2, 8, 128), 2)

    def merge_stats(stats, offset, turn_result=True):
        top = functools.reduce(jnp.maximum, stats)
        shift = lax.rem(128 - offset, 128)
        factors = [jnp.exp(s - top) for s in stats]
        den = sum(f * pltpu.roll(s, 64, 2) for f, s in zip(factors, stats))
        merged = jnp.where(lane < 64, top, pltpu.roll(den, 64, 2))
        if turn_result:
            merged = pltpu.roll(merged, shift, 2)
        return merged, [pltpu.roll(f, shift, 2) for f in factors]

    def spread(factor, lane_index):
        return jnp.broadcast_to(factor[:, lane_index:lane_index + 1], (8, 128))

    pending = {}

    def block(axis, position, lo, hi):
        sel = [slice(None)] * 3
        sel[axis] = position
        return u_ref.at[(pl.ds(lo, hi - lo),) + tuple(sel)]

    for colour in range(3):
        axis = ORDERS[colour][0]
        ends = (UNIT_LO[colour], UNIT_MID[colour], UNIT_HI[colour])
        far = peer_coord(axis, 2)
        for side, step in enumerate(RING):
            peer, near = peer_id(axis, step), peer_coord(axis, step)
            lo, hi = ends[side], ends[side + 1]
            pending[colour, side, 'stats'] = send(st_ref.at[pl.ds(colour, 2)], q1.at[colour, side], peer)
            pending[colour, side, 'relay'] = send(block(axis, far, lo, hi), relay.at[pl.ds(lo, hi - lo)], peer)
            lo, hi = ends[1 - side], ends[2 - side]
            pending[colour, side, 'near'] = send(block(axis, near, lo, hi), r1.at[0, pl.ds(lo, hi - lo)], peer)

    def ring_sum(colour, lo, hi, position, factors, arrays, store):
        axis = ORDERS[colour][0]
        first, second = [a for a in range(3) if a != axis]
        for i in range(4):
            for j in range(4):
                where = HEAD_STRIDE[first] * i + HEAD_STRIDE[second] * j
                at = [None] * 3
                at[axis], at[first], at[second] = position, i, j
                for bt in range(lo // 4, (hi - 1) // 4 + 1):
                    fb = [spread(f[bt - colour], where) for f in factors]
                    for unit in range(max(lo, bt * 4), min(hi, bt * 4 + 4)):
                        total = fb[0] * u_ref[unit, at[0], at[1], at[2]]
                        for f, array in zip(fb[1:], arrays):
                            total = total + f * array[unit, i, j]
                        store[unit, i, j] = total

    for colour in range(3):
        axis = ORDERS[colour][0]
        ends = (UNIT_LO[colour], UNIT_MID[colour], UNIT_HI[colour])
        for side, step in enumerate(RING):
            pending[colour, side, 'stats'].wait_recv()
            lo, hi = ends[side], ends[side + 1]
            peer, near = peer_id(axis, step), peer_coord(axis, step)
            pending[colour, side, 'relay'].wait_recv()
            merged, factors = merge_stats([st_ref[pl.ds(colour, 2)], q1[colour, side]], near * HEAD_STRIDE[axis], False)
            q0[colour, side] = merged
            ring_sum(colour, lo, hi, near, factors, [relay], passed)
            pending[colour, side, 'sum stats'] = send(q0.at[colour, side], q1.at[colour, 2 + side], peer)
            pending[colour, side, 'sum'] = send(passed.at[pl.ds(lo, hi - lo)], r1.at[1, pl.ds(lo, hi - lo)], peer)

    load_uv.wait()
    pick = lax.broadcasted_iota(jnp.int32, (64, 8, 128), 1) == lax.rem(head, 8)

    def pick_rows(i, carry):
        rows = pl.ds(pl.multiple_of(i * 64, 64), 64)
        wuv_h[rows, :] = jnp.sum(jnp.where(pick, wuv_v[rows].astype(f32), 0.0), axis=1).astype(bf16)
        return carry

    lax.fori_loop(0, 8, pick_rows, 0)

    for colour in range(3):
        order = ORDERS[colour]
        axis, axis2 = order[:2]
        lo, hi = UNIT_LO[colour], UNIT_HI[colour]
        ends = (lo, UNIT_MID[colour], hi)
        first, second = [a for a in range(3) if a != axis]
        for side in range(2):
            pending[colour, 1 - side, 'near'].wait_recv()
            pending[colour, side, 'sum stats'].wait_recv()
            pending[colour, side, 'sum'].wait_recv()
            stats = [st_ref[pl.ds(colour, 2)], q1[colour, 1 - side], q1[colour, 2 + side]]
            merged, factors = merge_stats(stats, coord[axis] * HEAD_STRIDE[axis])
            ring_sum(colour, ends[side], ends[side + 1], coord[axis], factors, [r1.at[0], r1.at[1]], v1)
        s1[colour] = merged
        for step in SEND_ORDER:
            pc = peer_coord(axis2, step)
            sel = (pc, slice(None)) if axis2 == first else (slice(None), pc)
            a = send(v1.at[(pl.ds(lo, hi - lo),) + sel], r2.at[step - 1, pl.ds(lo, hi - lo)], peer_id(axis2, step))
            b = send(s1.at[colour], q2.at[colour, step - 1], peer_id(axis2, step))
            pending[colour, step] = (a, b)

    for colour in range(3):
        order = ORDERS[colour]
        axis, axis2, axis3 = order
        lo, hi = UNIT_LO[colour], UNIT_HI[colour]
        first, second = [a for a in range(3) if a != axis]
        for step in WAIT_ORDER:
            for copy in pending[colour, step]:
                copy.wait_recv()
        stats = [s1[colour]] + [q2[colour, i] for i in range(3)]
        merged, factors = merge_stats(stats, coord[axis2] * HEAD_STRIDE[axis2])
        s2[colour] = merged
        for i in range(4):
            at = (coord[axis2], i) if axis2 == first else (i, coord[axis2])
            for bt in range(lo // 4, (hi - 1) // 4 + 1):
                fb = [spread(f[bt - colour], HEAD_STRIDE[axis3] * i) for f in factors]
                for unit in range(max(lo, bt * 4), min(hi, bt * 4 + 4)):
                    total = fb[0] * v1[unit, at[0], at[1]]
                    for k in range(3):
                        total = total + fb[k + 1] * r2[k, unit, i]
                    v2[unit, i] = total
        for step in SEND_ORDER:
            a = send(v2.at[pl.ds(lo, hi - lo), peer_coord(axis3, step)], r3.at[step - 1, pl.ds(lo, hi - lo)], peer_id(axis3, step))
            b = send(s2.at[colour], q3.at[colour, step - 1], peer_id(axis3, step))
            pending[colour, step] = (a, b)

    units = [None] * 16
    den = [None] * 16
    for colour in range(3):
        axis3 = ORDERS[colour][2]
        lo, hi = UNIT_LO[colour], UNIT_HI[colour]
        for step in WAIT_ORDER:
            for copy in pending[colour, step]:
                copy.wait_recv()
        stats = [s2[colour]] + [q3[colour, i] for i in range(3)]
        merged, factors = merge_stats(stats, coord[axis3] * HEAD_STRIDE[axis3])
        for bt in range(lo // 4, (hi - 1) // 4 + 1):
            fb = [spread(f[bt - colour], 0) for f in factors]
            dn = spread(merged[bt - colour], 64)
            for unit in range(max(lo, bt * 4), min(hi, bt * 4 + 4)):
                total = fb[0] * v2[unit, coord[axis3]]
                for k in range(3):
                    total = total + fb[k + 1] * r3[k, unit]
                units[unit] = total / dn
    o_lat = jnp.concatenate(
        [jnp.concatenate([units[bt * 4 + kt] for kt in range(4)], axis=1) for bt in range(4)], axis=0).astype(jnp.bfloat16)
    o_head = jnp.dot(o_lat, wuv_h[...], preferred_element_type=jnp.float32).astype(jnp.bfloat16)
    load_out.wait()
    def project(half):
        for cg in range(4):
            columns = pl.ds(pl.multiple_of((half * 4 + cg) * 640, 128), 640)
            part = jnp.dot(o_head, wout_v[:, columns], preferred_element_type=f32)
            y_buf[half, :, cg] = part.reshape(4, 8, 640)

    project(1 - tp)
    pair = send(y_buf.at[1 - tp], y_in, {'tp': 1 - tp})
    project(tp)
    pair.wait_recv()
    y_in[...] = y_in[...] + y_buf[tp]

    for colour in range(2):
        cols = pl.ds(OUT_LO[colour], OUT_HI[colour] - OUT_LO[colour])
        axis = colour
        for step in SEND_ORDER:
            pc = peer_coord(axis, step)
            src = y_in.at[pc, :, :, cols] if axis == 0 else y_in.at[:, pc, :, cols]
            pending[colour, step] = send(src, t1.at[step - 1, :, :, cols], peer_id(axis, step))
    for colour in range(2):
        cols = pl.ds(OUT_LO[colour], OUT_HI[colour] - OUT_LO[colour])
        axis, axis2 = colour, 1 - colour
        for step in WAIT_ORDER:
            pending[colour, step].wait_recv()
        for i in range(4):
            own = y_in[x, i, :, cols] if axis == 0 else y_in[i, y, :, cols]
            p1[i, :, cols] = own + sum(t1[k, i, :, cols] for k in range(3))
        for step in SEND_ORDER:
            pending[colour, step] = send(
                p1.at[peer_coord(axis2, step), :, cols], t2.at[step - 1, :, cols], peer_id(axis2, step))
    for colour in range(2):
        cols = pl.ds(OUT_LO[colour], OUT_HI[colour] - OUT_LO[colour])
        axis2 = 1 - colour
        for step in WAIT_ORDER:
            pending[colour, step].wait_recv()
        p2[:, cols] = p1[coord[axis2], :, cols] + sum(t2[k, :, cols] for k in range(3))

    for step in SEND_ORDER:
        pending[0, step] = send(p2, zbuf.at[z], peer_id(2, step))
    zbuf[z] = p2[...]
    for step in WAIT_ORDER:
        pending[0, step].wait_recv()
    g_buf[tp, x, y] = (zbuf[0] + zbuf[1]) + (zbuf[2] + zbuf[3])

    for colour in range(2):
        cols = pl.ds(OUT_LO[colour], OUT_HI[colour] - OUT_LO[colour])
        axis2 = 1 - colour
        mine = g_buf.at[tp, x, y, :, cols]
        for step in SEND_ORDER:
            pending[colour, step] = send(mine, mine, peer_id(axis2, step))
    for colour in range(2):
        cols = pl.ds(OUT_LO[colour], OUT_HI[colour] - OUT_LO[colour])
        axis = colour
        for step in WAIT_ORDER:
            pending[colour, step].wait_recv()
        mine = g_buf.at[tp, x, :, :, cols] if axis == 0 else g_buf.at[tp, :, y, :, cols]
        for step in SEND_ORDER:
            pending[colour, step] = send(mine, mine, peer_id(axis, step))
    pairs = []
    for colour in range(2):
        cols = pl.ds(OUT_LO[colour], OUT_HI[colour] - OUT_LO[colour])
        for step in WAIT_ORDER:
            pending[colour, step].wait_recv()
        mine = g_buf.at[tp, :, :, :, cols]
        pairs.append(send(mine, mine, {'tp': 1 - tp}))
    for pair in pairs:
        pair.wait_recv()
    for half in range(2):
        for cg in range(4):
            base = (half * 4 + cg) * 640
            out_ref[:, base:base + 640] = g_buf[half, :, cg].reshape(32, 640)
    for copy in started:
        copy.wait_send()


N_SENDS = 96


def tail(u_parts, stats, w_uv, w_out):
    parts = u_parts.shape[:3]
    cols = (8, 640)
    grid = parts[1:]
    vmem = pl.BlockSpec(memory_space=pltpu.VMEM)
    hbm = pl.BlockSpec(memory_space=pltpu.HBM)
    return pl.pallas_call(
        tail_kernel,
        out_shape=jax.ShapeDtypeStruct((32, 5120), f32),
        in_specs=[vmem, vmem, hbm, hbm],
        out_specs=vmem,
        scratch_shapes=[
            pltpu.VMEM(parts + TILE, f32),
            pltpu.VMEM(parts + TILE, f32),
            pltpu.VMEM((2,) + parts + TILE, f32),
            pltpu.VMEM(parts + TILE, f32),
            pltpu.VMEM((3,) + parts[:2] + TILE, f32),
            pltpu.VMEM(parts[:2] + TILE, f32),
            pltpu.VMEM((3,) + parts[:1] + TILE, f32),
            pltpu.VMEM((3, 2) + TILE, f32),
            pltpu.VMEM((3, 2) + TILE, f32),
            pltpu.VMEM((3, 2, 2) + TILE, f32),
            pltpu.VMEM((3, 4, 2) + TILE, f32),
            pltpu.VMEM((3, 3, 2) + TILE, f32),
            pltpu.VMEM((3, 3, 2) + TILE, f32),
            pltpu.VMEM((512,) + TILE, bf16),
            pltpu.VMEM((512, 128), bf16),
            pltpu.VMEM((128, 5120), bf16),
            pltpu.VMEM((2,) + grid + cols, f32),
            pltpu.VMEM(grid + cols, f32),
            pltpu.VMEM((3, 4) + cols, f32),
            pltpu.VMEM((3,) + cols, f32),
            pltpu.VMEM((4,) + cols, f32),
            pltpu.VMEM(cols, f32),
            pltpu.VMEM((4,) + cols, f32),
            pltpu.VMEM((2,) + grid + cols, f32),
            pltpu.SemaphoreType.DMA((N_SENDS,)),
            pltpu.SemaphoreType.DMA((N_SENDS,)),
            pltpu.SemaphoreType.DMA((2,)),
        ],
        compiler_params=pltpu.CompilerParams(collective_id=0, has_side_effects=True, vmem_limit_bytes=TAIL_VMEM),
        name='tail',
    )(u_parts, stats, w_uv, w_out)


def solution(mesh):
    row_spec = P('dp', None)
    cache_spec = P('dp', 'sp', None)
    head_spec = P(None, 'tp', None)
    in_specs = (row_spec, cache_spec, cache_spec, P('dp'), P(), P(), P(), P(), head_spec, head_spec, head_spec, P('tp', None))
    out_specs = (row_spec, cache_spec, cache_spec)

    def local_step(hidden, lat_cache, rope_cache, positions, w_dq, gain_q, w_dkv, gain_kv, w_uq, w_uk, w_uv, w_out):
        seq_local = lat_cache.shape[1]
        score_scale = YARN_MSCALE ** 2 / math.sqrt(w_uq.shape[2])
        cos_t, sin_t = rope_tables(positions, rope_cache.shape[2])
        q_abs, q_rope, lat_new, rope_new = front(hidden, gain_q, gain_kv, cos_t, sin_t, w_dkv, w_dq, w_uk, w_uq)
        base = (lax.axis_index('sp') * seq_local).reshape(1)
        lat_all, rope_all, u_parts, stats = attend(
            base, positions, q_abs, q_rope, lat_cache, rope_cache.transpose(0, 2, 1), lat_new, rope_new, score_scale)
        u_parts = u_parts.reshape(16, 4, 4, 4, 8, 128)
        attn_out = tail(u_parts, stats, w_uv, w_out)
        out = (hidden.astype(f32) + attn_out).astype(bf16)
        return out, lat_all, rope_all.transpose(0, 2, 1)

    return jax.shard_map(local_step, mesh=mesh, in_specs=in_specs, out_specs=out_specs, check_vma=False)
```
